256 devices in a mesh: dp: 32 (over z, x_hi, core), owner: 8 (over x_lo, y).
Axes of the slice: x: 4 (x_hi: 2, x_lo: 2; x = x_hi * 2 + x_lo), y: 4, z: 8, core: 2. Of those that a mesh axis runs over, the one named last changes fastest.
Arguments:
- edge_in: bfloat16 [8, 65536, 512], P(None, ('dp', 'owner')), may hold values from -256 to 256
- edge_grad: bfloat16 [8, 65536, 512], P(None, ('dp', 'owner')), may hold values from -1.1953125 to 1.1953125
- row_mask: int32 [8, 65536], P(None, ('dp', 'owner')), may hold values 0 or 1
- layer_at: int32 [8], replicated, may hold values from 0 to 7, each once
Outputs:
- update: bfloat16 [8, 512, 512], P('owner')
The draws below stay inside these ranges and needn't reach their ends.
Inputs may be any that keep to these rules, and one draw needn't show every extreme that they name: `layer_at`: every layer number appears once.
All inputs are finite; a program needn't handle non-finite values. No bound on the sum of `row_mask` on one device may be relied on, other than what follows from the above.
Results may differ from the reference program's by a relative error of at most 0.0085.
Values may be sent and summed in bfloat16 or wider, within the bound.
No kernel may reach another device: no remote copies, remote signals or barrier semaphores. Data moves between devices by JAX's collectives and lax.ppermute only.
A program may use at most 64 MiB of HBM per device.

```python
import math
import jax
import jax.numpy as jnp
from jax import lax

D = 512
LAYERS = 8
ROWS_DEV = 256
ROWS_ALL = 65536
ITERS = 4


def draw_edge_in(key, part):
    base = jax.random.fold_in(key, 11)
    key_a, key_b = jax.random.split(base, 2)
    normal_part = jnp.clip(jax.random.normal(key_a, (LAYERS, ROWS_ALL, D), jnp.float32), -6.0, 6.0)
    unit = jax.random.uniform(key_b, (LAYERS, ROWS_ALL, 1), jnp.float32)
    scale = jnp.exp(unit * jnp.log(10.0))
    values = scale * normal_part
    return jnp.clip(values, -256.0, 256.0).astype(jnp.bfloat16)


def plant(entries, stream_key, least, largest):
    extent = entries.shape
    index_at = [jax.random.randint(jax.random.fold_in(stream_key, axis), (), 0, extent[axis]) for axis in range(len(extent))]
    entries = entries.at[tuple(index_at)].set(least)
    longest = extent.index(max(extent))
    index_at[longest] = (index_at[longest] + 1) % extent[longest]
    return entries.at[tuple(index_at)].set(largest)


def steps_of(own_key, shape, cuts, least, largest):
    def one(dim, parts):
        steps = jax.random.uniform(jax.random.fold_in(jax.random.fold_in(own_key, 6), dim), (parts,), jnp.float32, least / len(cuts), largest / len(cuts))
        return jnp.repeat(jnp.exp(steps), shape[dim] // parts).reshape((-1,) + (1,) * (len(shape) - dim - 1))

    gain = one(*cuts[0])
    for cut in cuts[1:]:
        gain = gain * one(*cut)
    return gain


def normal_values(stream_key, shape, deviation, bound, cuts=(), held_as=jnp.bfloat16):
    values = deviation * jax.random.normal(stream_key, shape, jnp.float32)
    if cuts:
        values = values * steps_of(stream_key, shape, cuts, -0.22, 0.18)
    return jnp.clip(values, -bound, bound).astype(held_as)


def setup_inputs(seed: int = 0) -> dict:
    key_list = jax.random.split(jax.random.key(seed), 5)
    return {
        "edge_in": draw_edge_in(jax.random.fold_in(key_list[4], 71), 0),
        "edge_grad": normal_values(key_list[1], (LAYERS, ROWS_ALL, D), 0.2, 1.1953125, ((1, 256),)),
        "row_mask": plant((jax.random.randint(key_list[2], (LAYERS, ROWS_ALL), 0, 2) < 1).astype(jnp.int32), jax.random.fold_in(key_list[2], 1), 0, 1),
        "layer_at": jax.random.permutation(key_list[3], LAYERS).astype(jnp.int32),
    }


def newton(factor):
    eye = jnp.eye(D, dtype=jnp.float32)
    damped = factor + jnp.trace(factor) * (0.05 / D) * eye
    size_sq = jnp.sqrt(jnp.sum(damped * damped) + 1e-06)
    approx = eye / size_sq
    for step in range(ITERS):
        inner = jnp.matmul(damped, approx, precision=lax.Precision.HIGHEST)
        approx = 2.0 * approx - jnp.matmul(approx, inner, precision=lax.Precision.HIGHEST)
    return approx

def precondition(packed):
    factor_in, factor_out, grad = packed
    inv_in = newton(factor_in)
    inv_out = newton(factor_out)
    left = jnp.matmul(inv_in, grad, precision=lax.Precision.HIGHEST)
    return jnp.matmul(left, inv_out, precision=lax.Precision.HIGHEST)

def reference(edge_in, edge_grad, row_mask, layer_at):
    scale_factor = 1.0 / ROWS_ALL
    scale_grad = 1.0 / math.sqrt(ROWS_ALL)

    def add_block(index, carry):
        total_in, total_out, total_grad = carry
        start = index * ROWS_DEV
        inputs = lax.dynamic_slice_in_dim(edge_in, start, ROWS_DEV, 1).astype(jnp.float32)
        grads = lax.dynamic_slice_in_dim(edge_grad, start, ROWS_DEV, 1).astype(jnp.float32)
        weights = lax.dynamic_slice_in_dim(row_mask, start, ROWS_DEV, 1).astype(jnp.float32)[..., None]
        kept_in = inputs * weights
        kept_grad = grads * weights
        term_in = (jnp.einsum('lrd,lre->lde', kept_in, kept_in) * scale_factor).astype(jnp.bfloat16)
        term_out = (jnp.einsum('lrd,lre->lde', kept_grad, kept_grad) * scale_factor).astype(jnp.bfloat16)
        term_grad = (jnp.einsum('lrd,lre->lde', inputs, grads) * scale_grad).astype(jnp.bfloat16)
        term_in, term_out, term_grad = lax.optimization_barrier((term_in, term_out, term_grad))
        return (total_in + term_in.astype(jnp.float32), total_out + term_out.astype(jnp.float32), total_grad + term_grad.astype(jnp.float32))
    zeros = jnp.zeros((LAYERS, D, D), jnp.float32)
    factor_in, factor_out, grad = lax.fori_loop(0, ROWS_ALL // ROWS_DEV, add_block, (zeros, zeros, zeros))
    picked = (jnp.take(factor_in, layer_at, axis=0), jnp.take(factor_out, layer_at, axis=0), jnp.take(grad, layer_at, axis=0))
    update = lax.map(precondition, picked)
    return update.astype(jnp.bfloat16)
```

```python
import math

import jax
import jax.numpy as jnp
from jax import lax
from jax.experimental import pallas as pl
from jax.experimental.pallas import tpu as pltpu
from jax.sharding import Mesh
from jax.sharding import PartitionSpec as P

ITERS = 4
DP = ("dp_0", "dp_1", "dp_2")
DP_OWNER = ("dp_0", "dp_1", "dp_2", "owner")
MASK_ROWS = 8
TILE = 128


def upper_tiles(count):
    return [(i, j) for i in range(count) for j in range(i, count)]


def pack_kernel(at_ref, in_ref, grad_ref, mask_ref, out_ref):
    rows = in_ref.shape[1]
    width = in_ref.shape[2]
    out_ref[0, :rows, :] = in_ref[0]
    out_ref[0, rows : 2 * rows, :] = grad_ref[0]
    line = mask_ref[pl.ds(at_ref[pl.program_id(0)], 1), :].astype(jnp.float32)
    spare = jnp.zeros((MASK_ROWS, width - rows), jnp.float32)
    wide = jnp.concatenate([jnp.broadcast_to(line, (MASK_ROWS, rows)), spare], axis=1)
    out_ref[0, 2 * rows :, :] = wide.astype(jnp.bfloat16)


def pack(edge_in, edge_grad, row_mask, layer_at):
    layers, rows, width = edge_in.shape
    lines = 2 * rows + MASK_ROWS
    return pl.pallas_call(
        pack_kernel,
        out_shape=jax.ShapeDtypeStruct((layers, lines, width), jnp.bfloat16),
        grid_spec=pltpu.PrefetchScalarGridSpec(
            num_scalar_prefetch=1,
            grid=(layers,),
            in_specs=[
                pl.BlockSpec((1, rows, width), lambda s, at: (at[s], 0, 0)),
                pl.BlockSpec((1, rows, width), lambda s, at: (at[s], 0, 0)),
                pl.BlockSpec((layers, rows), lambda s, at: (0, 0)),
            ],
            out_specs=pl.BlockSpec((1, lines, width), lambda s, at: (s, 0, 0)),
        ),
    )(layer_at, edge_in, edge_grad, row_mask)


def gram_kernel(scale_factor, scale_grad, rows, held_ref, out_ref, in_acc, out_acc, grad_acc):
    step = pl.program_id(0)
    inputs = jnp.concatenate([held_ref[k, :rows, :] for k in range(held_ref.shape[0])], axis=0)
    grads = jnp.concatenate(
        [held_ref[k, rows : 2 * rows, :] for k in range(held_ref.shape[0])], axis=0
    )
    weights = jnp.concatenate(
        [held_ref[k, 2 * rows : 2 * rows + 1, :rows] for k in range(held_ref.shape[0])], axis=1
    )
    in_turned = inputs.T
    grad_turned = grads.T
    term_in = jnp.dot(in_turned * weights, inputs, preferred_element_type=jnp.float32)
    term_out = jnp.dot(grad_turned * weights, grads, preferred_element_type=jnp.float32)
    term_grad = jnp.dot(in_turned, grads, preferred_element_type=jnp.float32)

    @pl.when(step == 0)
    def _():
        in_acc[...] = term_in
        out_acc[...] = term_out
        grad_acc[...] = term_grad

    @pl.when(step > 0)
    def _():
        in_acc[...] += term_in
        out_acc[...] += term_out
        grad_acc[...] += term_grad

    @pl.when(step == pl.num_programs(0) - 1)
    def _():
        count = in_acc.shape[0] // TILE
        spot = 0
        for acc, scale, tiles in (
            (in_acc, scale_factor, upper_tiles(count)),
            (out_acc, scale_factor, upper_tiles(count)),
            (grad_acc, scale_grad, [(i, j) for i in range(count) for j in range(count)]),
        ):
            for i, j in tiles:
                tile = acc[i * TILE : (i + 1) * TILE, j * TILE : (j + 1) * TILE] * scale
                out_ref[spot : spot + TILE, :] = tile.astype(jnp.bfloat16)
                spot += TILE


def packed_lines(width):
    count = width // TILE
    return (count * (count + 1) + count * count) * TILE


def gram(held, rows, width, rows_all):
    sources, lines, _ = held.shape
    many = 2
    kernel = lambda *refs: gram_kernel(1.0 / rows_all, 1.0 / math.sqrt(rows_all), rows, *refs)
    return pl.pallas_call(
        kernel,
        name="gram",
        out_shape=jax.ShapeDtypeStruct((packed_lines(width), TILE), jnp.bfloat16),
        grid=(sources // many,),
        in_specs=[pl.BlockSpec((many, lines, width), lambda s: (s, 0, 0))],
        out_specs=pl.BlockSpec((packed_lines(width), TILE), lambda s: (0, 0)),
        scratch_shapes=[pltpu.VMEM((width, width), jnp.float32)] * 3,
    )(held)


def total_kernel(arrived_ref, copies_ref):
    whole = arrived_ref[0].astype(jnp.float32)
    for k in range(1, arrived_ref.shape[0]):
        whole += arrived_ref[k].astype(jnp.float32)
    low = whole.astype(jnp.bfloat16)
    for k in range(copies_ref.shape[0]):
        copies_ref[k] = low


def total_copies(arrived):
    return pl.pallas_call(
        total_kernel,
        name="total",
        out_shape=jax.ShapeDtypeStruct(arrived.shape, arrived.dtype),
        in_specs=[pl.BlockSpec(memory_space=pltpu.VMEM)],
        out_specs=pl.BlockSpec(memory_space=pltpu.VMEM),
    )(arrived)


def newton_kernel(width, packed_ref, out_ref, in_ref, grad_out_ref, mid_ref):
    count = width // TILE
    tiles = upper_tiles(count)
    diagonal = (
        lax.broadcasted_iota(jnp.int32, (TILE, TILE), 0)
        == lax.broadcasted_iota(jnp.int32, (TILE, TILE), 1)
    )
    starts = []
    for ref, base in ((in_ref, 0), (grad_out_ref, len(tiles) * TILE)):
        trace = jnp.float32(0.0)
        for k, (i, j) in enumerate(tiles):
            tile = packed_ref[base + k * TILE : base + (k + 1) * TILE, :].astype(jnp.float32)
            ref[i * TILE : (i + 1) * TILE, j * TILE : (j + 1) * TILE] = tile
            if i == j:
                trace += jnp.sum(jnp.where(diagonal, tile, 0.0))
            else:
                ref[j * TILE : (j + 1) * TILE, i * TILE : (i + 1) * TILE] = tile.T
        shift = jnp.where(diagonal, trace * (0.05 / width), 0.0)
        for i in range(count):
            at = slice(i * TILE, (i + 1) * TILE)
            ref[at, at] += shift
        whole = ref[...]
        scale = lax.rsqrt(jnp.sum(whole * whole) + 1e-06)
        ref[...] = whole * scale
        starts.append(scale)
    base = 2 * len(tiles) * TILE
    for i in range(count):
        for j in range(count):
            k = base + (i * count + j) * TILE
            mid_ref[i * TILE : (i + 1) * TILE, j * TILE : (j + 1) * TILE] = packed_ref[
                k : k + TILE, :
            ].astype(jnp.float32)

    def dot(a, b):
        return jnp.dot(a, b, preferred_element_type=jnp.float32)

    for step in range(ITERS):
        left = in_ref[...]
        right = grad_out_ref[...]
        left_low = left.astype(jnp.bfloat16)
        right_low = right.astype(jnp.bfloat16)
        mid = mid_ref[...]
        mid = 2.0 * mid - dot(left_low, mid.astype(jnp.bfloat16))
        mid = 2.0 * mid - dot(mid.astype(jnp.bfloat16), right_low)
        if step < ITERS - 1:
            mid_ref[...] = mid
            in_ref[...] = 2.0 * left - dot(left_low, left_low)
            grad_out_ref[...] = 2.0 * right - dot(right_low, right_low)
        else:
            out_ref[...] = (mid * starts[0] * starts[1]).astype(jnp.bfloat16)


def newton(packed, width):
    return pl.pallas_call(
        lambda *refs: newton_kernel(width, *refs),
        name="newton",
        out_shape=jax.ShapeDtypeStruct((width, width), jnp.bfloat16),
        in_specs=[pl.BlockSpec(memory_space=pltpu.VMEM)],
        out_specs=pl.BlockSpec(memory_space=pltpu.VMEM),
        scratch_shapes=[pltpu.VMEM((width, width), jnp.float32)] * 3,
    )(packed)


def local(edge_in, edge_grad, row_mask, layer_at):
    rows = edge_in.shape[1]
    width = edge_in.shape[2]
    replicas = lax.axis_size(DP)
    rows_all = rows * replicas * lax.axis_size("owner")
    sent = pack(edge_in, edge_grad, row_mask, layer_at)
    held = lax.all_to_all(sent, "owner", 0, 0, tiled=True)
    partial = gram(held, rows, width, rows_all)
    pieces = partial.reshape(replicas, -1, TILE)
    arrived = lax.all_to_all(pieces, DP, 0, 0, tiled=True)
    whole = lax.all_to_all(total_copies(arrived), DP, 0, 0, tiled=True)
    update = newton(whole.reshape(-1, TILE), width)
    return update[None]


def solution(mesh):
    split = Mesh(
        mesh.devices.reshape(8, 2, 2, mesh.shape["owner"]), ("dp_0", "dp_1", "dp_2", "owner")
    )
    placed = (P(None, DP_OWNER, None), P(None, DP_OWNER, None), P(None, DP_OWNER), P())
    return jax.shard_map(
        local, mesh=split, in_specs=placed, out_specs=P("owner", None, None), check_vma=False
    )
```

```python
import math

import jax
import jax.numpy as jnp
from jax import lax
from jax.experimental import pallas as pl
from jax.experimental.pallas import tpu as pltpu
from jax.sharding import Mesh
from jax.sharding import PartitionSpec as P

ITERS = 4
DP = ("dp_0", "dp_1", "dp_2")
DP_OWNER = ("dp_0", "dp_1", "dp_2", "owner")
MASK_ROWS = 8
TILE = 128


def upper_tiles(count):
    return [(i, j) for i in range(count) for j in range(i, count)]


def pack_kernel(at_ref, mask_ref, in_ref, grad_ref, out_ref, wide_ref, sem):
    layers, rows, width = in_ref.shape
    copies = []
    for s in range(layers):
        layer = at_ref[s]
        copies.append(
            pltpu.make_async_copy(in_ref.at[layer], out_ref.at[s, pl.ds(0, rows)], sem.at[s, 0])
        )
        copies.append(
            pltpu.make_async_copy(
                grad_ref.at[layer], out_ref.at[s, pl.ds(rows, rows)], sem.at[s, 1]
            )
        )
    for copy in copies:
        copy.start()
    wide_ref[...] = jnp.zeros(wide_ref.shape, wide_ref.dtype)
    for s in range(layers):
        line = mask_ref[pl.ds(at_ref[s], 1), :].astype(jnp.float32)
        wide_ref[s, :, :rows] = jnp.broadcast_to(line, (MASK_ROWS, rows)).astype(jnp.bfloat16)
    last = [
        pltpu.make_async_copy(
            wide_ref.at[s], out_ref.at[s, pl.ds(2 * rows, MASK_ROWS)], sem.at[s, 2]
        )
        for s in range(layers)
    ]
    for copy in last:
        copy.start()
    for copy in copies + last:
        copy.wait()


def pack(edge_in, edge_grad, row_mask, layer_at):
    layers, rows, width = edge_in.shape
    lines = 2 * rows + MASK_ROWS
    anywhere = pl.BlockSpec(memory_space=pl.ANY)
    return pl.pallas_call(
        pack_kernel,
        name="pack",
        out_shape=jax.ShapeDtypeStruct((layers, lines, width), jnp.bfloat16),
        in_specs=[
            pl.BlockSpec(memory_space=pltpu.SMEM),
            pl.BlockSpec(memory_space=pltpu.VMEM),
            anywhere,
            anywhere,
        ],
        out_specs=anywhere,
        scratch_shapes=[
            pltpu.VMEM((layers, MASK_ROWS, width), jnp.bfloat16),
            pltpu.SemaphoreType.DMA((layers, 3)),
        ],
    )(layer_at, row_mask, edge_in, edge_grad)


def half_tiles(count):
    upper = upper_tiles(count)
    half = count // 2
    return [
        [("in", i, j) for i, j in upper]
        + [("grad", i, j) for i in range(half) for j in range(count)],
        [("out", i, j) for i, j in upper]
        + [("grad", i, j) for i in range(half, count) for j in range(count)],
    ]


def half_lines(width):
    return len(half_tiles(width // TILE)[0]) * TILE


def gram_kernel(
    scale_factor, scale_grad, rows, core_ref, held_ref, mine_ref, theirs_ref,
    in_all, grad_all, mask_all, in_turned, grad_turned, accs, sem,
):
    sources = held_ref.shape[0]
    width = held_ref.shape[2]
    half = width // 2
    copies = []
    for k in range(sources):
        at = pl.ds(k * rows, rows)
        copies.append(
            [
                pltpu.make_async_copy(
                    held_ref.at[k, pl.ds(2 * rows, MASK_ROWS)], mask_all.at[k], sem.at[k, 2]
                ),
                pltpu.make_async_copy(held_ref.at[k, pl.ds(0, rows)], in_all.at[at], sem.at[k, 0]),
                pltpu.make_async_copy(
                    held_ref.at[k, pl.ds(rows, rows)], grad_all.at[at], sem.at[k, 1]
                ),
            ]
        )
    for group in copies:
        for copy in group:
            copy.start()
    for k, group in enumerate(copies):
        for copy in group:
            copy.wait()
        at = slice(k * rows, (k + 1) * rows)
        in_turned[:, at] = in_all[at, :].T
        grad_turned[:, at] = grad_all[at, :].T
    weights = jnp.concatenate([mask_all[k, :1, :rows] for k in range(sources)], axis=1)

    def dot(a, b):
        return jnp.dot(a, b, preferred_element_type=jnp.float32)

    accs[2] = dot(in_turned[...], grad_all[...])
    for n, turned, plain in ((0, in_turned, in_all), (1, grad_turned, grad_all)):
        kept = turned[...] * weights
        accs[n, :half, :] = dot(kept[:half], plain[...])
        accs[n, half:, half:] = dot(kept[half:], plain[:, half:])
    place = {"in": (0, scale_factor), "out": (1, scale_factor), "grad": (2, scale_grad)}
    halves = half_tiles(width // TILE)

    def write(ref, tiles):
        for spot, (kind, i, j) in enumerate(tiles):
            n, scale = place[kind]
            tile = accs[n, i * TILE : (i + 1) * TILE, j * TILE : (j + 1) * TILE] * scale
            ref[spot * TILE : (spot + 1) * TILE, :] = tile.astype(ref.dtype)

    for core in range(2):

        @pl.when(core_ref[0] == core)
        def _(core=core):
            write(mine_ref, halves[core])
            write(theirs_ref, halves[1 - core])


def gram(core, held, rows, width, rows_all):
    sources = held.shape[0]
    lines = half_lines(width)
    kernel = lambda *refs: gram_kernel(1.0 / rows_all, 1.0 / math.sqrt(rows_all), rows, *refs)
    inside = pl.BlockSpec(memory_space=pltpu.VMEM)
    return pl.pallas_call(
        kernel,
        name="gram",
        compiler_params=pltpu.CompilerParams(vmem_limit_bytes=28 << 20),
        out_shape=(
            jax.ShapeDtypeStruct((lines, TILE), jnp.float32),
            jax.ShapeDtypeStruct((lines, TILE), jnp.bfloat16),
        ),
        in_specs=[pl.BlockSpec(memory_space=pltpu.SMEM), pl.BlockSpec(memory_space=pl.ANY)],
        out_specs=(inside, inside),
        scratch_shapes=[
            pltpu.VMEM((sources * rows, width), jnp.bfloat16),
            pltpu.VMEM((sources * rows, width), jnp.bfloat16),
            pltpu.VMEM((sources, MASK_ROWS, width), jnp.bfloat16),
            pltpu.VMEM((width, sources * rows), jnp.bfloat16),
            pltpu.VMEM((width, sources * rows), jnp.bfloat16),
            pltpu.VMEM((3, width, width), jnp.float32),
            pltpu.SemaphoreType.DMA((sources, 3)),
        ],
    )(core, held)


def pair_kernel(mine_ref, other_ref, out_ref):
    out_ref[...] = (mine_ref[...] + other_ref[...].astype(jnp.float32)).astype(jnp.bfloat16)


def pair_sum(mine, other):
    inside = pl.BlockSpec(memory_space=pltpu.VMEM)
    return pl.pallas_call(
        pair_kernel,
        name="pair",
        compiler_params=pltpu.CompilerParams(vmem_limit_bytes=8 << 20),
        out_shape=jax.ShapeDtypeStruct(other.shape, other.dtype),
        in_specs=[inside, inside],
        out_specs=inside,
    )(mine, other)


def total_kernel(arrived_ref, copies_ref):
    whole = arrived_ref[0].astype(jnp.float32)
    for k in range(1, arrived_ref.shape[0]):
        whole += arrived_ref[k].astype(jnp.float32)
    low = whole.astype(jnp.bfloat16)
    for k in range(copies_ref.shape[0]):
        copies_ref[k] = low


def total_copies(arrived):
    return pl.pallas_call(
        total_kernel,
        name="total",
        compiler_params=pltpu.CompilerParams(vmem_limit_bytes=8 << 20),
        out_shape=jax.ShapeDtypeStruct(arrived.shape, arrived.dtype),
        in_specs=[pl.BlockSpec(memory_space=pltpu.VMEM)],
        out_specs=pl.BlockSpec(memory_space=pltpu.VMEM),
    )(arrived)


def newton_kernel(width, core_ref, own_ref, other_ref, out_ref, left_ref, right_ref, mid_ref):
    count = width // TILE
    halves = half_tiles(count)
    spots = {t: (h, k * TILE) for h in range(2) for k, t in enumerate(halves[h])}
    diagonal = (
        lax.broadcasted_iota(jnp.int32, (TILE, TILE), 0)
        == lax.broadcasted_iota(jnp.int32, (TILE, TILE), 1)
    )

    def unpack(h, ref):
        target = {"in": left_ref, "out": right_ref, "grad": mid_ref}
        for spot, (kind, i, j) in enumerate(halves[h]):
            tile = ref[spot * TILE : (spot + 1) * TILE, :].astype(jnp.float32)
            target[kind][i * TILE : (i + 1) * TILE, j * TILE : (j + 1) * TILE] = tile
            if kind != "grad" and i != j:
                target[kind][j * TILE : (j + 1) * TILE, i * TILE : (i + 1) * TILE] = tile.T

    for core in range(2):

        @pl.when(core_ref[0] == core)
        def _(core=core):
            unpack(core, own_ref)
            unpack(1 - core, other_ref)

    starts = []
    for ref in (left_ref, right_ref):
        trace = jnp.float32(0.0)
        for i in range(count):
            at = slice(i * TILE, (i + 1) * TILE)
            trace += jnp.sum(jnp.where(diagonal, ref[at, at], 0.0))
        shift = jnp.where(diagonal, trace * (0.05 / width), 0.0)
        for i in range(count):
            at = slice(i * TILE, (i + 1) * TILE)
            ref[at, at] += shift
        whole = ref[...]
        scale = lax.rsqrt(jnp.sum(whole * whole) + 1e-06)
        ref[...] = whole * scale
        starts.append(scale)

    def dot(a, b):
        return jnp.dot(a, b, preferred_element_type=jnp.float32)

    for step in range(ITERS):
        left = left_ref[...]
        right = right_ref[...]
        left_low = left.astype(jnp.bfloat16)
        right_low = right.astype(jnp.bfloat16)
        mid = mid_ref[...]
        mid = 2.0 * mid - dot(left_low, mid.astype(jnp.bfloat16))
        mid = 2.0 * mid - dot(mid.astype(jnp.bfloat16), right_low)
        if step < ITERS - 1:
            mid_ref[...] = mid
            left_ref[...] = 2.0 * left - dot(left_low, left_low)
            right_ref[...] = 2.0 * right - dot(right_low, right_low)
        else:
            out_ref[...] = (mid * starts[0] * starts[1]).astype(jnp.bfloat16)


def newton(core, own, other, width):
    inside = pl.BlockSpec(memory_space=pltpu.VMEM)
    return pl.pallas_call(
        lambda *refs: newton_kernel(width, *refs),
        name="newton",
        compiler_params=pltpu.CompilerParams(vmem_limit_bytes=16 << 20),
        out_shape=jax.ShapeDtypeStruct((width, width), jnp.bfloat16),
        in_specs=[pl.BlockSpec(memory_space=pltpu.SMEM), inside, inside],
        out_specs=inside,
        scratch_shapes=[pltpu.VMEM((width, width), jnp.float32)] * 3,
    )(core, own, other)


def local(edge_in, edge_grad, row_mask, layer_at):
    rows = edge_in.shape[1]
    width = edge_in.shape[2]
    far, pair = DP[:2], DP[2]
    replicas = lax.axis_size(far)
    rows_all = rows * lax.axis_size(DP) * lax.axis_size("owner")
    swap = [(0, 1), (1, 0)]
    core = lax.axis_index(pair).astype(jnp.int32).reshape(1)
    sent = pack(edge_in, edge_grad, row_mask, layer_at)
    held = lax.all_to_all(sent, "owner", 0, 0, tiled=True)
    mine, theirs = gram(core, held, rows, width, rows_all)
    pieces = pair_sum(mine, lax.ppermute(theirs, pair, swap)).reshape(replicas, -1, TILE)
    arrived = lax.all_to_all(pieces, far, 0, 0, tiled=True)
    own = lax.all_to_all(total_copies(arrived), far, 0, 0, tiled=True).reshape(-1, TILE)
    update = newton(core, own, lax.ppermute(own, pair, swap), width)
    return update[None]


def solution(mesh):
    split = Mesh(
        mesh.devices.reshape(8, 2, 2, mesh.shape["owner"]), ("dp_0", "dp_1", "dp_2", "owner")
    )
    placed = (P(None, DP_OWNER, None), P(None, DP_OWNER, None), P(None, DP_OWNER), P())
    return jax.shard_map(
        local, mesh=split, in_specs=placed, out_specs=P("owner", None, None), check_vma=False
    )
```

```python
import math

import jax
import jax.numpy as jnp
from jax import lax
from jax.experimental import pallas as pl
from jax.experimental.pallas import tpu as pltpu
from jax.sharding import Mesh
from jax.sharding import PartitionSpec as P

ITERS = 4
AXES = ("zh", "zl", "xh", "core", "xl", "yh", "yl")
CHIPS = ("zh", "zl", "xh", "xl", "yh", "yl")
OWNER = ("xl", "yh", "yl")
SIZES = {"zh": 4, "zl": 2, "xh": 2, "core": 2, "xl": 2, "yh": 2, "yl": 2}
STEPS = ((-1, -1, -1), (1, -1, 0), (-1, 0, 1), (0, 1, -1), (1, 0, 0), (0, 1, 0), (0, 0, 1))
PIECES = STEPS + ((0, 0, 0),)
MASK_ROWS = 8
TILE = 128


def upper_tiles(count):
    return [(i, j) for i in range(count) for j in range(i, count)]


def chip_index(x, y, z):
    return ((z * 2 + x // 2) * 2 + x % 2) * 4 + y


def step_pairs(step):
    dx, dy, dz = step
    return [
        (chip_index(x, y, z), chip_index((x + dx) % 4, (y + dy) % 4, (z + dz) % 8))
        for x in range(4)
        for y in range(4)
        for z in range(8)
    ]


def slot_towards(step):
    x = lax.axis_index("xl") + 4 + step[0]
    y = lax.axis_index("yl") + 4 + step[1]
    z = lax.axis_index("zl") + 4 + step[2]
    return lax.rem(x, 2) * 4 + lax.rem(z, 2) * 2 + lax.rem(y, 2)


def pack_kernel(rows, at_ref, mask_ref, in_ref, grad_ref, *rest):
    out_refs, sem = rest[:-1], rest[-1]
    copies = []
    layers = []
    for k, out_ref in enumerate(out_refs):
        layer = at_ref[slot_towards(PIECES[k])]
        layers.append(layer)
        copies.append(
            pltpu.make_async_copy(in_ref.at[layer], out_ref.at[pl.ds(0, rows)], sem.at[k, 0])
        )
        copies.append(
            pltpu.make_async_copy(grad_ref.at[layer], out_ref.at[pl.ds(rows, rows)], sem.at[k, 1])
        )
    for copy in copies:
        copy.start()
    for layer, out_ref in zip(layers, out_refs):
        line = mask_ref[pl.ds(layer, 1), :].astype(jnp.float32)
        spare = jnp.zeros((MASK_ROWS, out_ref.shape[1] - rows), jnp.float32)
        wide = jnp.concatenate([jnp.broadcast_to(line, (MASK_ROWS, rows)), spare], axis=1)
        out_ref[2 * rows :, :] = wide.astype(jnp.bfloat16)
    for copy in copies:
        copy.wait()


def pack(edge_in, edge_grad, row_mask, layer_at):
    _, rows, width = edge_in.shape
    piece = jax.ShapeDtypeStruct((2 * rows + MASK_ROWS, width), jnp.bfloat16)
    far = pl.BlockSpec(memory_space=pl.ANY)
    inside = pl.BlockSpec(memory_space=pltpu.VMEM)
    return pl.pallas_call(
        lambda *refs: pack_kernel(rows, *refs),
        name="pack",
        compiler_params=pltpu.CompilerParams(vmem_limit_bytes=60 << 20),
        out_shape=(piece,) * len(PIECES),
        in_specs=[pl.BlockSpec(memory_space=pltpu.SMEM), inside, far, far],
        out_specs=(inside,) * len(PIECES),
        scratch_shapes=[pltpu.SemaphoreType.DMA((len(PIECES), 2))],
    )(layer_at, row_mask, edge_in, edge_grad)


def half_tiles(count):
    upper = upper_tiles(count)
    half = count // 2
    return [
        [("in", i, j) for i, j in upper]
        + [("grad", i, j) for i in range(half) for j in range(count)],
        [("out", i, j) for i, j in upper]
        + [("grad", i, j) for i in range(half, count) for j in range(count)],
    ]


def half_lines(width):
    return len(half_tiles(width // TILE)[0]) * TILE


def gram_kernel(
    scale_factor, scale_grad, rows, core_ref, *rest
):
    sources = len(PIECES)
    held_refs = rest[:sources]
    mine_ref, theirs_ref = rest[sources : sources + 2]
    in_all, grad_all, mask_all, in_turned, grad_turned, accs, sem = rest[sources + 2 :]
    width = in_all.shape[1]
    half = width // 2
    copies = []
    for k, held in enumerate(held_refs):
        at = pl.ds(k * rows, rows)
        copies.append(
            (
                pltpu.make_async_copy(held.at[pl.ds(0, rows)], in_all.at[at], sem.at[k, 0]),
                pltpu.make_async_copy(held.at[pl.ds(rows, rows)], grad_all.at[at], sem.at[k, 1]),
                pltpu.make_async_copy(
                    held.at[pl.ds(2 * rows, MASK_ROWS)], mask_all.at[k], sem.at[k, 2]
                ),
            )
        )
    for group in copies:
        for copy in group:
            copy.start()
    for k, group in enumerate(copies):
        for copy in group:
            copy.wait()
        at = slice(k * rows, (k + 1) * rows)
        in_turned[:, at] = in_all[at, :].T
        grad_turned[:, at] = grad_all[at, :].T
    weights = jnp.concatenate([mask_all[k, :1, :rows] for k in range(sources)], axis=1)

    def dot(a, b):
        return jnp.dot(a, b, preferred_element_type=jnp.float32)

    accs[2] = dot(in_turned[...], grad_all[...])
    for n, turned, plain in ((0, in_turned, in_all), (1, grad_turned, grad_all)):
        kept = turned[...] * weights
        accs[n, :half, :] = dot(kept[:half], plain[...])
        accs[n, half:, half:] = dot(kept[half:], plain[:, half:])
    place = {"in": (0, scale_factor), "out": (1, scale_factor), "grad": (2, scale_grad)}
    halves = half_tiles(width // TILE)

    def write(ref, tiles):
        for spot, (kind, i, j) in enumerate(tiles):
            n, scale = place[kind]
            tile = accs[n, i * TILE : (i + 1) * TILE, j * TILE : (j + 1) * TILE] * scale
            ref[spot * TILE : (spot + 1) * TILE, :] = tile.astype(ref.dtype)

    for core in range(2):

        @pl.when(core_ref[0] == core)
        def _(core=core):
            write(mine_ref, halves[core])
            write(theirs_ref, halves[1 - core])


def gram(core, held, rows, rows_all):
    width = held[0].shape[1]
    lines = half_lines(width)
    depth = rows * len(held)
    kernel = lambda *refs: gram_kernel(1.0 / rows_all, 1.0 / math.sqrt(rows_all), rows, *refs)
    inside = pl.BlockSpec(memory_space=pltpu.VMEM)
    anywhere = pl.BlockSpec(memory_space=pl.ANY)
    return pl.pallas_call(
        kernel,
        name="gram",
        compiler_params=pltpu.CompilerParams(vmem_limit_bytes=28 << 20),
        out_shape=(
            jax.ShapeDtypeStruct((lines, TILE), jnp.float32),
            jax.ShapeDtypeStruct((lines, TILE), jnp.bfloat16),
        ),
        in_specs=[pl.BlockSpec(memory_space=pltpu.SMEM)] + [anywhere] * len(held),
        out_specs=(inside, inside),
        scratch_shapes=[
            pltpu.VMEM((depth, width), jnp.bfloat16),
            pltpu.VMEM((depth, width), jnp.bfloat16),
            pltpu.VMEM((len(held), MASK_ROWS, width), jnp.bfloat16),
            pltpu.VMEM((width, depth), jnp.bfloat16),
            pltpu.VMEM((width, depth), jnp.bfloat16),
            pltpu.VMEM((3, width, width), jnp.float32),
            pltpu.SemaphoreType.DMA((len(held), 3)),
        ],
    )(core, *held)


def pair_kernel(mine_ref, other_ref, out_ref):
    out_ref[...] = (mine_ref[...] + other_ref[...].astype(jnp.float32)).astype(jnp.bfloat16)


def pair_sum(mine, other):
    inside = pl.BlockSpec(memory_space=pltpu.VMEM)
    return pl.pallas_call(
        pair_kernel,
        name="pair",
        compiler_params=pltpu.CompilerParams(vmem_limit_bytes=8 << 20),
        out_shape=jax.ShapeDtypeStruct(other.shape, other.dtype),
        in_specs=[inside, inside],
        out_specs=inside,
    )(mine, other)


def total_kernel(arrived_ref, out_ref):
    whole = arrived_ref[0].astype(jnp.float32)
    for k in range(1, arrived_ref.shape[0]):
        whole += arrived_ref[k].astype(jnp.float32)
    out_ref[...] = whole.astype(jnp.bfloat16)


def total(arrived):
    return pl.pallas_call(
        total_kernel,
        name="total",
        compiler_params=pltpu.CompilerParams(vmem_limit_bytes=8 << 20),
        out_shape=jax.ShapeDtypeStruct(arrived.shape[1:], arrived.dtype),
        in_specs=[pl.BlockSpec(memory_space=pltpu.VMEM)],
        out_specs=pl.BlockSpec(memory_space=pltpu.VMEM),
    )(arrived)


def copies_kernel(one_ref, out_ref):
    for k in range(out_ref.shape[0]):
        out_ref[k] = one_ref[...]


def copies(one, count):
    return pl.pallas_call(
        copies_kernel,
        name="copies",
        compiler_params=pltpu.CompilerParams(vmem_limit_bytes=8 << 20),
        out_shape=jax.ShapeDtypeStruct((count, *one.shape), one.dtype),
        in_specs=[pl.BlockSpec(memory_space=pltpu.VMEM)],
        out_specs=pl.BlockSpec(memory_space=pltpu.VMEM),
    )(one)


def newton_kernel(width, core_ref, own_ref, other_ref, out_ref, left_ref, right_ref, mid_ref):
    count = width // TILE
    halves = half_tiles(count)
    spots = {t: (h, k * TILE) for h in range(2) for k, t in enumerate(halves[h])}
    diagonal = (
        lax.broadcasted_iota(jnp.int32, (TILE, TILE), 0)
        == lax.broadcasted_iota(jnp.int32, (TILE, TILE), 1)
    )

    def unpack(h, ref):
        target = {"in": left_ref, "out": right_ref, "grad": mid_ref}
        for spot, (kind, i, j) in enumerate(halves[h]):
            tile = ref[spot * TILE : (spot + 1) * TILE, :].astype(jnp.float32)
            target[kind][i * TILE : (i + 1) * TILE, j * TILE : (j + 1) * TILE] = tile
            if kind != "grad" and i != j:
                target[kind][j * TILE : (j + 1) * TILE, i * TILE : (i + 1) * TILE] = tile.T

    for core in range(2):

        @pl.when(core_ref[0] == core)
        def _(core=core):
            unpack(core, own_ref)
            unpack(1 - core, other_ref)

    starts = []
    for ref in (left_ref, right_ref):
        trace = jnp.float32(0.0)
        for i in range(count):
            at = slice(i * TILE, (i + 1) * TILE)
            trace += jnp.sum(jnp.where(diagonal, ref[at, at], 0.0))
        shift = jnp.where(diagonal, trace * (0.05 / width), 0.0)
        for i in range(count):
            at = slice(i * TILE, (i + 1) * TILE)
            ref[at, at] += shift
        whole = ref[...]
        scale = lax.rsqrt(jnp.sum(whole * whole) + 1e-06)
        ref[...] = whole * scale
        starts.append(scale)

    def dot(a, b):
        return jnp.dot(a, b, preferred_element_type=jnp.float32)

    for step in range(ITERS):
        left = left_ref[...]
        right = right_ref[...]
        left_low = left.astype(jnp.bfloat16)
        right_low = right.astype(jnp.bfloat16)
        mid = mid_ref[...]
        mid = 2.0 * mid - dot(left_low, mid.astype(jnp.bfloat16))
        mid = 2.0 * mid - dot(mid.astype(jnp.bfloat16), right_low)
        if step < ITERS - 1:
            mid_ref[...] = mid
            left_ref[...] = 2.0 * left - dot(left_low, left_low)
            right_ref[...] = 2.0 * right - dot(right_low, right_low)
        else:
            out_ref[...] = (mid * starts[0] * starts[1]).astype(jnp.bfloat16)


def newton(core, own, other, width):
    inside = pl.BlockSpec(memory_space=pltpu.VMEM)
    return pl.pallas_call(
        lambda *refs: newton_kernel(width, *refs),
        name="newton",
        compiler_params=pltpu.CompilerParams(vmem_limit_bytes=16 << 20),
        out_shape=jax.ShapeDtypeStruct((width, width), jnp.bfloat16),
        in_specs=[pl.BlockSpec(memory_space=pltpu.SMEM), inside, inside],
        out_specs=inside,
        scratch_shapes=[pltpu.VMEM((width, width), jnp.float32)] * 3,
    )(core, own, other)


def local(edge_in, edge_grad, row_mask, layer_at):
    rows = edge_in.shape[1]
    width = edge_in.shape[2]
    rows_all = rows * lax.axis_size(AXES)
    swap = [(0, 1), (1, 0)]
    turn = [(0, 0), (1, 2), (2, 1), (3, 3)]
    core = lax.axis_index("core").astype(jnp.int32).reshape(1)
    sent = pack(edge_in, edge_grad, row_mask, layer_at)
    held = [lax.ppermute(p, CHIPS, step_pairs(step)) for p, step in zip(sent, STEPS)]
    mine, theirs = gram(core, held + [sent[-1]], rows, rows_all)
    pieces = pair_sum(mine, lax.ppermute(theirs, "core", swap))
    summed_over = ("zh", "xh", "yh")
    count = lax.axis_size(summed_over)
    arrived = lax.all_to_all(pieces.reshape(count, -1, TILE), summed_over, 0, 0, tiled=True)
    moved = lax.ppermute(total(arrived), ("zl", "yh"), turn)
    own = lax.all_to_all(copies(moved, count), ("zh", "xh", "zl"), 0, 0, tiled=True)
    own = own.reshape(-1, TILE)
    update = newton(core, own, lax.ppermute(own, "core", swap), width)
    return update[None]


def solution(mesh):
    split = Mesh(mesh.devices.reshape(tuple(SIZES[a] for a in AXES)), AXES)
    placed = (P(None, AXES, None), P(None, AXES, None), P(None, AXES), P())
    return jax.shard_map(
        local, mesh=split, in_specs=placed, out_specs=P(OWNER, None, None), check_vma=False
    )
```

```python
import math

import jax
import jax.numpy as jnp
from jax import lax
from jax.experimental import pallas as pl
from jax.experimental.pallas import tpu as pltpu
from jax.sharding import Mesh
from jax.sharding import PartitionSpec as P

ITERS = 4
AXES = ("zh", "zl", "xh", "core", "xl", "yh", "yl")
CHIPS = ("zh", "zl", "xh", "xl", "yh", "yl")
OWNER = ("xl", "yh", "yl")
SIZES = {"zh": 4, "zl": 2, "xh": 2, "core": 2, "xl": 2, "yh": 2, "yl": 2}
FIRST = ((-1, -1, -1), (1, 0, 0), (0, 1, 0), (0, 0, 1))
SECOND = ((1, -1, 0), (-1, 0, 1), (0, 1, -1))
HERE = (0, 0, 0)
MASK_ROWS = 8
TILE = 128


def upper_tiles(count):
    return [(i, j) for i in range(count) for j in range(i, count)]


def chip_index(x, y, z):
    return ((z * 2 + x // 2) * 2 + x % 2) * 4 + y


def step_pairs(step):
    dx, dy, dz = step
    return [
        (chip_index(x, y, z), chip_index((x + dx) % 4, (y + dy) % 4, (z + dz) % 8))
        for x in range(4)
        for y in range(4)
        for z in range(8)
    ]


def slot_towards(step):
    x = lax.axis_index("xl") + 4 + step[0]
    y = lax.axis_index("yl") + 4 + step[1]
    z = lax.axis_index("zl") + 4 + step[2]
    return lax.rem(x, 2) * 4 + lax.rem(z, 2) * 2 + lax.rem(y, 2)


def pack_kernel(steps, rows, at_ref, mask_ref, in_ref, grad_ref, *rest):
    out_refs, sem = rest[:-1], rest[-1]
    copies = []
    layers = []
    for k, out_ref in enumerate(out_refs):
        layer = at_ref[slot_towards(steps[k])]
        layers.append(layer)
        copies.append(
            pltpu.make_async_copy(in_ref.at[layer], out_ref.at[pl.ds(0, rows)], sem.at[k, 0])
        )
        copies.append(
            pltpu.make_async_copy(grad_ref.at[layer], out_ref.at[pl.ds(rows, rows)], sem.at[k, 1])
        )
    for copy in copies:
        copy.start()
    for layer, out_ref in zip(layers, out_refs):
        line = mask_ref[pl.ds(layer, 1), :].astype(jnp.float32)
        spare = jnp.zeros((MASK_ROWS, out_ref.shape[1] - rows), jnp.float32)
        wide = jnp.concatenate([jnp.broadcast_to(line, (MASK_ROWS, rows)), spare], axis=1)
        out_ref[2 * rows :, :] = wide.astype(jnp.bfloat16)
    for copy in copies:
        copy.wait()


def pack(steps, edge_in, edge_grad, row_mask, layer_at):
    _, rows, width = edge_in.shape
    piece = jax.ShapeDtypeStruct((2 * rows + MASK_ROWS, width), jnp.bfloat16)
    far = pl.BlockSpec(memory_space=pl.ANY)
    inside = pl.BlockSpec(memory_space=pltpu.VMEM)
    return pl.pallas_call(
        lambda *refs: pack_kernel(steps, rows, *refs),
        name="pack",
        compiler_params=pltpu.CompilerParams(vmem_limit_bytes=60 << 20),
        out_shape=(piece,) * len(steps),
        in_specs=[pl.BlockSpec(memory_space=pltpu.SMEM), inside, far, far],
        out_specs=(inside,) * len(steps),
        scratch_shapes=[pltpu.SemaphoreType.DMA((len(steps), 2))],
    )(layer_at, row_mask, edge_in, edge_grad)


def half_tiles(count):
    upper = upper_tiles(count)
    half = count // 2
    return [
        [("in", i, j) for i, j in upper]
        + [("grad", i, j) for i in range(half) for j in range(count)],
        [("out", i, j) for i, j in upper]
        + [("grad", i, j) for i in range(half, count) for j in range(count)],
    ]


def half_lines(width):
    return len(half_tiles(width // TILE)[0]) * TILE


def gram_kernel(pieces, rows, finish, refs):
    held_refs, refs = refs[:pieces], refs[pieces:]
    in_all, grad_all, mask_all, in_turned, grad_turned, sem = refs[-6:]
    width = in_all.shape[1]
    half = width // 2
    copies = []
    for k, held in enumerate(held_refs):
        at = pl.ds(k * rows, rows)
        copies.append(
            (
                pltpu.make_async_copy(held.at[pl.ds(0, rows)], in_all.at[at], sem.at[k, 0]),
                pltpu.make_async_copy(held.at[pl.ds(rows, rows)], grad_all.at[at], sem.at[k, 1]),
                pltpu.make_async_copy(
                    held.at[pl.ds(2 * rows, MASK_ROWS)], mask_all.at[k], sem.at[k, 2]
                ),
            )
        )
    for group in copies:
        for copy in group:
            copy.start()
    for k, group in enumerate(copies):
        for copy in group:
            copy.wait()
        at = slice(k * rows, (k + 1) * rows)
        in_turned[:, at] = in_all[at, :].T
        grad_turned[:, at] = grad_all[at, :].T
    weights = jnp.concatenate([mask_all[k, :1, :rows] for k in range(pieces)], axis=1)

    def dot(a, b):
        return jnp.dot(a, b, preferred_element_type=jnp.float32)

    finish(
        refs[:-6],
        2,
        ((slice(0, width), slice(0, width), dot(in_turned[...], grad_all[...])),),
    )
    for n, turned, plain in ((0, in_turned, in_all), (1, grad_turned, grad_all)):
        kept = turned[...] * weights
        upper, lower = slice(0, half), slice(half, width)
        finish(
            refs[:-6],
            n,
            (
                (upper, slice(0, width), dot(kept[:half], plain[...])),
                (lower, lower, dot(kept[half:], plain[:, half:])),
            ),
        )


def gram_scratch(pieces, rows, width):
    depth = pieces * rows
    return [
        pltpu.VMEM((depth, width), jnp.bfloat16),
        pltpu.VMEM((depth, width), jnp.bfloat16),
        pltpu.VMEM((pieces, MASK_ROWS, width), jnp.bfloat16),
        pltpu.VMEM((width, depth), jnp.bfloat16),
        pltpu.VMEM((width, depth), jnp.bfloat16),
        pltpu.SemaphoreType.DMA((pieces, 3)),
    ]


def gram_first(held, rows):
    width = held[0].shape[1]
    anywhere = pl.BlockSpec(memory_space=pl.ANY)

    def keep(refs, n, blocks):
        for at, to, value in blocks:
            refs[0][n, at, to] = value

    return pl.pallas_call(
        lambda *refs: gram_kernel(len(held), rows, keep, refs),
        name="gram_first",
        compiler_params=pltpu.CompilerParams(vmem_limit_bytes=28 << 20),
        out_shape=jax.ShapeDtypeStruct((3, width, width), jnp.float32),
        in_specs=[anywhere] * len(held),
        out_specs=pl.BlockSpec(memory_space=pltpu.VMEM),
        scratch_shapes=gram_scratch(len(held), rows, width),
    )(*held)


def gram_last(core, sums, held, rows, rows_all):
    width = held[0].shape[1]
    lines = half_lines(width)
    halves = half_tiles(width // TILE)
    scales = (1.0 / rows_all, 1.0 / rows_all, 1.0 / math.sqrt(rows_all))
    kinds = ("in", "out", "grad")
    inside = pl.BlockSpec(memory_space=pltpu.VMEM)
    anywhere = pl.BlockSpec(memory_space=pl.ANY)

    def kernel(*refs):
        pieces = len(held)
        core_ref, sums_ref = refs[:2]

        def write(outs, n, blocks):
            core_ref, mine_ref, theirs_ref, whole_ref = outs
            for at, to, value in blocks:
                whole_ref[n, at, to] = sums_ref[n, at, to] + value
            for core in range(2):

                @pl.when(core_ref[0] == core)
                def _(core=core):
                    for ref, tiles in ((mine_ref, halves[core]), (theirs_ref, halves[1 - core])):
                        for spot, (kind, i, j) in enumerate(tiles):
                            if kind == kinds[n]:
                                across = slice(j * TILE, (j + 1) * TILE)
                                tile = whole_ref[n, i * TILE : (i + 1) * TILE, across] * scales[n]
                                ref[spot * TILE : (spot + 1) * TILE, :] = tile.astype(ref.dtype)

        rest = refs[2 + pieces :]
        gram_kernel(
            pieces, rows, lambda outs, n, blocks: write((core_ref, *outs), n, blocks),
            refs[2 : 2 + pieces] + rest,
        )

    return pl.pallas_call(
        kernel,
        name="gram_last",
        compiler_params=pltpu.CompilerParams(vmem_limit_bytes=28 << 20),
        out_shape=(
            jax.ShapeDtypeStruct((lines, TILE), jnp.float32),
            jax.ShapeDtypeStruct((lines, TILE), jnp.bfloat16),
        ),
        in_specs=[pl.BlockSpec(memory_space=pltpu.SMEM), inside] + [anywhere] * len(held),
        out_specs=(inside, inside),
        scratch_shapes=[pltpu.VMEM((3, width, width), jnp.float32)]
        + gram_scratch(len(held), rows, width),
    )(core, sums, *held)


def pair_kernel(mine_ref, other_ref, out_ref):
    out_ref[...] = (mine_ref[...] + other_ref[...].astype(jnp.float32)).astype(jnp.bfloat16)


def pair_sum(mine, other):
    inside = pl.BlockSpec(memory_space=pltpu.VMEM)
    return pl.pallas_call(
        pair_kernel,
        name="pair",
        compiler_params=pltpu.CompilerParams(vmem_limit_bytes=8 << 20),
        out_shape=jax.ShapeDtypeStruct(other.shape, other.dtype),
        in_specs=[inside, inside],
        out_specs=inside,
    )(mine, other)


def total_kernel(arrived_ref, out_ref):
    whole = arrived_ref[0].astype(jnp.float32)
    for k in range(1, arrived_ref.shape[0]):
        whole += arrived_ref[k].astype(jnp.float32)
    out_ref[...] = whole.astype(jnp.bfloat16)


def total(arrived):
    return pl.pallas_call(
        total_kernel,
        name="total",
        compiler_params=pltpu.CompilerParams(vmem_limit_bytes=8 << 20),
        out_shape=jax.ShapeDtypeStruct(arrived.shape[1:], arrived.dtype),
        in_specs=[pl.BlockSpec(memory_space=pltpu.VMEM)],
        out_specs=pl.BlockSpec(memory_space=pltpu.VMEM),
    )(arrived)


def copies_kernel(one_ref, out_ref):
    for k in range(out_ref.shape[0]):
        out_ref[k] = one_ref[...]


def copies(one, count):
    return pl.pallas_call(
        copies_kernel,
        name="copies",
        compiler_params=pltpu.CompilerParams(vmem_limit_bytes=8 << 20),
        out_shape=jax.ShapeDtypeStruct((count, *one.shape), one.dtype),
        in_specs=[pl.BlockSpec(memory_space=pltpu.VMEM)],
        out_specs=pl.BlockSpec(memory_space=pltpu.VMEM),
    )(one)


def newton_kernel(width, core_ref, own_ref, other_ref, out_ref, left_ref, right_ref, mid_ref):
    count = width // TILE
    halves = half_tiles(count)
    spots = {t: (h, k * TILE) for h in range(2) for k, t in enumerate(halves[h])}
    diagonal = (
        lax.broadcasted_iota(jnp.int32, (TILE, TILE), 0)
        == lax.broadcasted_iota(jnp.int32, (TILE, TILE), 1)
    )

    def unpack(h, ref):
        target = {"in": left_ref, "out": right_ref, "grad": mid_ref}
        for spot, (kind, i, j) in enumerate(halves[h]):
            tile = ref[spot * TILE : (spot + 1) * TILE, :].astype(jnp.float32)
            target[kind][i * TILE : (i + 1) * TILE, j * TILE : (j + 1) * TILE] = tile
            if kind != "grad" and i != j:
                target[kind][j * TILE : (j + 1) * TILE, i * TILE : (i + 1) * TILE] = tile.T

    for core in range(2):

        @pl.when(core_ref[0] == core)
        def _(core=core):
            unpack(core, own_ref)
            unpack(1 - core, other_ref)

    starts = []
    for ref in (left_ref, right_ref):
        trace = jnp.float32(0.0)
        for i in range(count):
            at = slice(i * TILE, (i + 1) * TILE)
            trace += jnp.sum(jnp.where(diagonal, ref[at, at], 0.0))
        shift = jnp.where(diagonal, trace * (0.05 / width), 0.0)
        for i in range(count):
            at = slice(i * TILE, (i + 1) * TILE)
            ref[at, at] += shift
        whole = ref[...]
        scale = lax.rsqrt(jnp.sum(whole * whole) + 1e-06)
        ref[...] = whole * scale
        starts.append(scale)

    def dot(a, b):
        return jnp.dot(a, b, preferred_element_type=jnp.float32)

    for step in range(ITERS):
        left = left_ref[...]
        right = right_ref[...]
        left_low = left.astype(jnp.bfloat16)
        right_low = right.astype(jnp.bfloat16)
        mid = mid_ref[...]
        mid = 2.0 * mid - dot(left_low, mid.astype(jnp.bfloat16))
        mid = 2.0 * mid - dot(mid.astype(jnp.bfloat16), right_low)
        if step < ITERS - 1:
            mid_ref[...] = mid
            left_ref[...] = 2.0 * left - dot(left_low, left_low)
            right_ref[...] = 2.0 * right - dot(right_low, right_low)
        else:
            out_ref[...] = (mid * starts[0] * starts[1]).astype(jnp.bfloat16)


def newton(core, own, other, width):
    inside = pl.BlockSpec(memory_space=pltpu.VMEM)
    return pl.pallas_call(
        lambda *refs: newton_kernel(width, *refs),
        name="newton",
        compiler_params=pltpu.CompilerParams(vmem_limit_bytes=16 << 20),
        out_shape=jax.ShapeDtypeStruct((width, width), jnp.bfloat16),
        in_specs=[pl.BlockSpec(memory_space=pltpu.SMEM), inside, inside],
        out_specs=inside,
        scratch_shapes=[pltpu.VMEM((width, width), jnp.float32)] * 3,
    )(core, own, other)


def local(edge_in, edge_grad, row_mask, layer_at):
    rows = edge_in.shape[1]
    width = edge_in.shape[2]
    rows_all = rows * lax.axis_size(AXES)
    swap = [(0, 1), (1, 0)]
    turn = [(0, 0), (1, 2), (2, 1), (3, 3)]
    core = lax.axis_index("core").astype(jnp.int32).reshape(1)
    args = (edge_in, edge_grad, row_mask, layer_at)

    def exchanged(sent, steps):
        return [lax.ppermute(p, CHIPS, step_pairs(step)) for p, step in zip(sent, steps)]

    early = exchanged(pack(FIRST, *args), FIRST)
    *sent, kept = pack(SECOND + (HERE,), *args)
    late = exchanged(sent, SECOND)
    sums = gram_first([kept] + early, rows)
    mine, theirs = gram_last(core, sums, late, rows, rows_all)
    pieces = pair_sum(mine, lax.ppermute(theirs, "core", swap))
    summed_over = ("zh", "xh", "yh")
    count = lax.axis_size(summed_over)
    arrived = lax.all_to_all(pieces.reshape(count, -1, TILE), summed_over, 0, 0, tiled=True)
    moved = lax.ppermute(total(arrived), ("zl", "yh"), turn)
    own = lax.all_to_all(copies(moved, count), ("zh", "xh", "zl"), 0, 0, tiled=True)
    own = own.reshape(-1, TILE)
    update = newton(core, own, lax.ppermute(own, "core", swap), width)
    return update[None]


def solution(mesh):
    split = Mesh(mesh.devices.reshape(tuple(SIZES[a] for a in AXES)), AXES)
    placed = (P(None, AXES, None), P(None, AXES, None), P(None, AXES), P())
    return jax.shard_map(
        local, mesh=split, in_specs=placed, out_specs=P(OWNER, None, None), check_vma=False
    )
```

```python
import math

import jax
import jax.numpy as jnp
from jax import lax
from jax.experimental import pallas as pl
from jax.experimental.pallas import tpu as pltpu
from jax.sharding import Mesh
from jax.sharding import PartitionSpec as P

ITERS = 4
AXES = ("zh", "zl", "xh", "core", "xl", "yh", "yl")
CHIPS = ("zh", "zl", "xh", "xl", "yh", "yl")
OWNER = ("xl", "yh", "yl")
SIZES = {"zh": 4, "zl": 2, "xh": 2, "core": 2, "xl": 2, "yh": 2, "yl": 2}
FIRST = ((1, 0, 0), (0, 1, 0), (0, 0, 1), (-1, -1, -1))
SECOND = ((1, -1, 0), (-1, 0, 1), (0, 1, -1))
HERE = (0, 0, 0)
MASK_ROWS = 8
TILE = 128


def upper_tiles(count):
    return [(i, j) for i in range(count) for j in range(i, count)]


def chip_index(x, y, z):
    return ((z * 2 + x // 2) * 2 + x % 2) * 4 + y


def step_pairs(step):
    dx, dy, dz = step
    return [
        (chip_index(x, y, z), chip_index((x + dx) % 4, (y + dy) % 4, (z + dz) % 8))
        for x in range(4)
        for y in range(4)
        for z in range(8)
    ]


def slot_towards(step):
    x = lax.axis_index("xl") + 4 + step[0]
    y = lax.axis_index("yl") + 4 + step[1]
    z = lax.axis_index("zl") + 4 + step[2]
    return lax.rem(x, 2) * 4 + lax.rem(z, 2) * 2 + lax.rem(y, 2)


def pack_kernel(steps, rows, at_ref, mask_ref, in_ref, grad_ref, *rest):
    out_refs, sem = rest[:-1], rest[-1]
    copies = []
    layers = []
    for k, out_ref in enumerate(out_refs):
        layer = at_ref[slot_towards(steps[k])]
        layers.append(layer)
        copies.append(
            pltpu.make_async_copy(in_ref.at[layer], out_ref.at[pl.ds(0, rows)], sem.at[k, 0])
        )
        copies.append(
            pltpu.make_async_copy(grad_ref.at[layer], out_ref.at[pl.ds(rows, rows)], sem.at[k, 1])
        )
    for copy in copies:
        copy.start()
    for layer, out_ref in zip(layers, out_refs):
        line = mask_ref[pl.ds(layer, 1), :].astype(jnp.float32)
        spare = jnp.zeros((MASK_ROWS, out_ref.shape[1] - rows), jnp.float32)
        wide = jnp.concatenate([jnp.broadcast_to(line, (MASK_ROWS, rows)), spare], axis=1)
        out_ref[2 * rows :, :] = wide.astype(jnp.bfloat16)
    for copy in copies:
        copy.wait()


def pack(steps, edge_in, edge_grad, row_mask, layer_at):
    _, rows, width = edge_in.shape
    piece = jax.ShapeDtypeStruct((2 * rows + MASK_ROWS, width), jnp.bfloat16)
    far = pl.BlockSpec(memory_space=pl.ANY)
    inside = pl.BlockSpec(memory_space=pltpu.VMEM)
    return pl.pallas_call(
        lambda *refs: pack_kernel(steps, rows, *refs),
        name="pack",
        compiler_params=pltpu.CompilerParams(vmem_limit_bytes=60 << 20),
        out_shape=(piece,) * len(steps),
        in_specs=[pl.BlockSpec(memory_space=pltpu.SMEM), inside, far, far],
        out_specs=(inside,) * len(steps),
        scratch_shapes=[pltpu.SemaphoreType.DMA((len(steps), 2))],
    )(layer_at, row_mask, edge_in, edge_grad)


def half_tiles(count):
    upper = upper_tiles(count)
    half = count // 2
    return [
        [("in", i, j) for i, j in upper]
        + [("grad", i, j) for i in range(half) for j in range(count)],
        [("out", i, j) for i, j in upper]
        + [("grad", i, j) for i in range(half, count) for j in range(count)],
    ]


def half_lines(width):
    return len(half_tiles(width // TILE)[0]) * TILE


def gram_kernel(pieces, rows, finish, refs):
    held_refs, refs = refs[:pieces], refs[pieces:]
    in_all, grad_all, mask_all, in_turned, grad_turned, sem = refs[-6:]
    width = in_all.shape[1]
    half = width // 2
    copies = []
    for k, held in enumerate(held_refs):
        at = pl.ds(k * rows, rows)
        copies.append(
            (
                pltpu.make_async_copy(held.at[pl.ds(0, rows)], in_all.at[at], sem.at[k, 0]),
                pltpu.make_async_copy(held.at[pl.ds(rows, rows)], grad_all.at[at], sem.at[k, 1]),
                pltpu.make_async_copy(
                    held.at[pl.ds(2 * rows, MASK_ROWS)], mask_all.at[k], sem.at[k, 2]
                ),
            )
        )
    for group in copies:
        for copy in group:
            copy.start()
    for k, group in enumerate(copies):
        for copy in group:
            copy.wait()
        at = slice(k * rows, (k + 1) * rows)
        in_turned[:, at] = in_all[at, :].T
        grad_turned[:, at] = grad_all[at, :].T
    weights = jnp.concatenate([mask_all[k, :1, :rows] for k in range(pieces)], axis=1)

    def dot(a, b):
        return jnp.dot(a, b, preferred_element_type=jnp.float32)

    finish(
        refs[:-6],
        2,
        ((slice(0, width), slice(0, width), dot(in_turned[...], grad_all[...])),),
    )
    for n, turned, plain in ((0, in_turned, in_all), (1, grad_turned, grad_all)):
        kept = turned[...] * weights
        upper, lower = slice(0, half), slice(half, width)
        finish(
            refs[:-6],
            n,
            (
                (upper, slice(0, width), dot(kept[:half], plain[...])),
                (lower, lower, dot(kept[half:], plain[:, half:])),
            ),
        )


def gram_scratch(pieces, rows, width):
    depth = pieces * rows
    return [
        pltpu.VMEM((depth, width), jnp.bfloat16),
        pltpu.VMEM((depth, width), jnp.bfloat16),
        pltpu.VMEM((pieces, MASK_ROWS, width), jnp.bfloat16),
        pltpu.VMEM((width, depth), jnp.bfloat16),
        pltpu.VMEM((width, depth), jnp.bfloat16),
        pltpu.SemaphoreType.DMA((pieces, 3)),
    ]


def gram_some(held, rows, *before):
    width = held[0].shape[1]
    anywhere = pl.BlockSpec(memory_space=pl.ANY)
    inside = pl.BlockSpec(memory_space=pltpu.VMEM)

    def kernel(*refs):
        sums, refs = refs[: len(before)], refs[len(before) :]

        def keep(outs, n, blocks):
            for at, to, value in blocks:
                for ref in sums:
                    value = value + ref[n, at, to]
                outs[0][n, at, to] = value

        gram_kernel(len(held), rows, keep, refs)

    return pl.pallas_call(
        kernel,
        name="gram_some",
        compiler_params=pltpu.CompilerParams(vmem_limit_bytes=28 << 20),
        out_shape=jax.ShapeDtypeStruct((3, width, width), jnp.float32),
        in_specs=[inside] * len(before) + [anywhere] * len(held),
        out_specs=inside,
        scratch_shapes=gram_scratch(len(held), rows, width),
    )(*before, *held)


def gram_last(core, sums, held, rows, rows_all):
    width = held[0].shape[1]
    lines = half_lines(width)
    halves = half_tiles(width // TILE)
    scales = (1.0 / rows_all, 1.0 / rows_all, 1.0 / math.sqrt(rows_all))
    kinds = ("in", "out", "grad")
    inside = pl.BlockSpec(memory_space=pltpu.VMEM)
    anywhere = pl.BlockSpec(memory_space=pl.ANY)

    def kernel(*refs):
        pieces = len(held)
        core_ref, sums_ref = refs[:2]

        def write(outs, n, blocks):
            core_ref, mine_ref, theirs_ref, whole_ref = outs
            for at, to, value in blocks:
                whole_ref[n, at, to] = sums_ref[n, at, to] + value
            for core in range(2):

                @pl.when(core_ref[0] == core)
                def _(core=core):
                    for ref, tiles in ((mine_ref, halves[core]), (theirs_ref, halves[1 - core])):
                        for spot, (kind, i, j) in enumerate(tiles):
                            if kind == kinds[n]:
                                across = slice(j * TILE, (j + 1) * TILE)
                                tile = whole_ref[n, i * TILE : (i + 1) * TILE, across] * scales[n]
                                ref[spot * TILE : (spot + 1) * TILE, :] = tile.astype(ref.dtype)

        rest = refs[2 + pieces :]
        gram_kernel(
            pieces, rows, lambda outs, n, blocks: write((core_ref, *outs), n, blocks),
            refs[2 : 2 + pieces] + rest,
        )

    return pl.pallas_call(
        kernel,
        name="gram_last",
        compiler_params=pltpu.CompilerParams(vmem_limit_bytes=28 << 20),
        out_shape=(
            jax.ShapeDtypeStruct((lines, TILE), jnp.float32),
            jax.ShapeDtypeStruct((lines, TILE), jnp.bfloat16),
        ),
        in_specs=[pl.BlockSpec(memory_space=pltpu.SMEM), inside] + [anywhere] * len(held),
        out_specs=(inside, inside),
        scratch_shapes=[pltpu.VMEM((3, width, width), jnp.float32)]
        + gram_scratch(len(held), rows, width),
    )(core, sums, *held)


def pair_kernel(mine_ref, other_ref, out_ref):
    out_ref[...] = (mine_ref[...] + other_ref[...].astype(jnp.float32)).astype(jnp.bfloat16)


def pair_sum(mine, other):
    inside = pl.BlockSpec(memory_space=pltpu.VMEM)
    return pl.pallas_call(
        pair_kernel,
        name="pair",
        compiler_params=pltpu.CompilerParams(vmem_limit_bytes=8 << 20),
        out_shape=jax.ShapeDtypeStruct(other.shape, other.dtype),
        in_specs=[inside, inside],
        out_specs=inside,
    )(mine, other)


def total_kernel(arrived_ref, out_ref):
    count = arrived_ref.shape[0]
    for slot in range(2):
        sources = [k for k in range(count) if k // 4 % 2 == slot]
        whole = arrived_ref[sources[0]].astype(jnp.float32)
        for k in sources[1:]:
            whole += arrived_ref[k].astype(jnp.float32)
        low = whole.astype(jnp.bfloat16)
        for k in range(count):
            if k % 2 == slot:
                out_ref[k] = low


def total(arrived):
    return pl.pallas_call(
        total_kernel,
        name="total",
        compiler_params=pltpu.CompilerParams(vmem_limit_bytes=8 << 20),
        out_shape=jax.ShapeDtypeStruct(arrived.shape, arrived.dtype),
        in_specs=[pl.BlockSpec(memory_space=pltpu.VMEM)],
        out_specs=pl.BlockSpec(memory_space=pltpu.VMEM),
    )(arrived)


def diagonal_of_tile():
    rows = lax.broadcasted_iota(jnp.int32, (TILE, TILE), 0)
    return rows == lax.broadcasted_iota(jnp.int32, (TILE, TILE), 1)


def low_dot(a, b):
    return jnp.dot(a, b, preferred_element_type=jnp.float32)


def powers(tiles_ref, whole_ref, put):
    width = whole_ref.shape[0]
    count = width // TILE
    diagonal = diagonal_of_tile()
    trace = jnp.zeros((TILE, TILE), jnp.float32)
    for spot, (i, j) in enumerate(upper_tiles(count)):
        tile = tiles_ref[spot * TILE : (spot + 1) * TILE, :].astype(jnp.float32)
        whole_ref[i * TILE : (i + 1) * TILE, j * TILE : (j + 1) * TILE] = tile
        if i == j:
            trace += jnp.where(diagonal, tile, 0.0)
        else:
            whole_ref[j * TILE : (j + 1) * TILE, i * TILE : (i + 1) * TILE] = tile.T
    shift = jnp.where(diagonal, jnp.sum(trace) * (0.05 / width), 0.0)
    for i in range(count):
        at = slice(i * TILE, (i + 1) * TILE)
        whole_ref[at, at] += shift
    whole = whole_ref[...]
    scale = lax.rsqrt(jnp.sum(whole * whole) + 1e-06)
    whole = whole * scale
    for step in range(ITERS):
        low = whole.astype(jnp.bfloat16)
        put(step, low)
        if step < ITERS - 1:
            whole = 2.0 * whole - low_dot(low, low)
    return scale


def own_powers_kernel(own_ref, out_ref, scale_ref, whole_ref):
    def put(step, low):
        out_ref[step] = low

    scale_ref[0] = powers(own_ref, whole_ref, put)


def own_powers(own, width):
    inside = pl.BlockSpec(memory_space=pltpu.VMEM)
    return pl.pallas_call(
        own_powers_kernel,
        name="own_powers",
        compiler_params=pltpu.CompilerParams(vmem_limit_bytes=12 << 20),
        out_shape=(
            jax.ShapeDtypeStruct((ITERS, width, width), jnp.bfloat16),
            jax.ShapeDtypeStruct((1,), jnp.float32),
        ),
        in_specs=[inside],
        out_specs=(inside, pl.BlockSpec(memory_space=pltpu.SMEM)),
        scratch_shapes=[pltpu.VMEM((width, width), jnp.float32)],
    )(own)


def newton_kernel(
    core_ref, scale_ref, mine_ref, own_ref, other_ref, out_ref, all_ref, whole_ref, mid_ref, sem
):
    width = whole_ref.shape[0]
    count = width // TILE
    core = core_ref[0]
    bring = pltpu.make_async_copy(mine_ref, all_ref.at[0], sem)
    bring.start()

    def put(step, low):
        all_ref[1, step] = low

    scale = powers(other_ref, whole_ref, put) * scale_ref[0]
    base = len(upper_tiles(count)) * TILE
    half = count // 2
    for part, ref in enumerate((own_ref, other_ref)):
        first = jnp.where(core == part, 0, half * TILE)
        for i in range(half):
            for j in range(count):
                spot = base + (i * count + j) * TILE
                at = pl.ds(pl.multiple_of(first + i * TILE, TILE), TILE)
                mid_ref[at, j * TILE : (j + 1) * TILE] = ref[spot : spot + TILE, :].astype(
                    jnp.float32
                )
    bring.wait()
    mid = mid_ref[...]
    for step in range(ITERS):
        mid = 2.0 * mid - low_dot(all_ref[core, step], mid.astype(jnp.bfloat16))
        mid = 2.0 * mid - low_dot(mid.astype(jnp.bfloat16), all_ref[1 - core, step])
    out_ref[...] = (mid * scale).astype(jnp.bfloat16)


def newton(core, scale, mine, own, other, width):
    inside = pl.BlockSpec(memory_space=pltpu.VMEM)
    scalars = pl.BlockSpec(memory_space=pltpu.SMEM)
    return pl.pallas_call(
        newton_kernel,
        name="newton",
        compiler_params=pltpu.CompilerParams(vmem_limit_bytes=20 << 20),
        out_shape=jax.ShapeDtypeStruct((width, width), jnp.bfloat16),
        in_specs=[scalars, scalars, pl.BlockSpec(memory_space=pl.ANY), inside, inside],
        out_specs=inside,
        scratch_shapes=[
            pltpu.VMEM((2, ITERS, width, width), jnp.bfloat16),
            pltpu.VMEM((width, width), jnp.float32),
            pltpu.VMEM((width, width), jnp.float32),
            pltpu.SemaphoreType.DMA,
        ],
    )(core, scale, mine, own, other)


def local(edge_in, edge_grad, row_mask, layer_at):
    rows = edge_in.shape[1]
    width = edge_in.shape[2]
    rows_all = rows * lax.axis_size(AXES)
    swap = [(0, 1), (1, 0)]
    core = lax.axis_index("core").astype(jnp.int32).reshape(1)
    args = (edge_in, edge_grad, row_mask, layer_at)

    def exchanged(sent, steps):
        return [lax.ppermute(p, CHIPS, step_pairs(step)) for p, step in zip(sent, steps)]

    early = exchanged(pack(FIRST, *args), FIRST)
    *sent, kept = pack(SECOND + (HERE,), *args)
    late = exchanged(sent, SECOND)
    sums = gram_some([kept] + early, rows)
    sums = gram_some(late[:-1], rows, sums)
    mine, theirs = gram_last(core, sums, late[-1:], rows, rows_all)
    pieces = pair_sum(mine, lax.ppermute(theirs, "core", swap))
    around = ("zh", "zl", "xh", "yh")
    blocks = pieces.reshape(lax.axis_size(around), -1, TILE)
    arrived = lax.all_to_all(blocks, around, 0, 0, tiled=True)
    own = lax.all_to_all(total(arrived), around, 0, 0, tiled=True).reshape(-1, TILE)
    other = lax.ppermute(own, "core", swap)
    low, scale = own_powers(own, width)
    update = newton(core, scale, low, own, other, width)
    return update[None]


def solution(mesh):
    split = Mesh(mesh.devices.reshape(tuple(SIZES[a] for a in AXES)), AXES)
    placed = (P(None, AXES, None), P(None, AXES, None), P(None, AXES), P())
    return jax.shard_map(
        local, mesh=split, in_specs=placed, out_specs=P(OWNER, None, None), check_vma=False
    )
```

```python
import math

import jax
import jax.numpy as jnp
from jax import lax
from jax.experimental import pallas as pl
from jax.experimental.pallas import tpu as pltpu
from jax.sharding import Mesh
from jax.sharding import PartitionSpec as P

ITERS = 4
AXES = ("zh", "zl", "xh", "core", "xl", "yh", "yl")
CHIPS = ("zh", "zl", "xh", "xl", "yh", "yl")
OWNER = ("xl", "yh", "yl")
SIZES = {"zh": 4, "zl": 2, "xh": 2, "core": 2, "xl": 2, "yh": 2, "yl": 2}
FIRST = ((1, 0, 0), (0, 1, 0), (0, 0, 1), (-1, -1, -1))
SECOND = ((1, -1, 0), (-1, 0, 1), (0, 1, -1))
HERE = (0, 0, 0)
MASK_ROWS = 8
TILE = 128


def upper_tiles(count):
    return [(i, j) for i in range(count) for j in range(i, count)]


def chip_index(x, y, z):
    return ((z * 2 + x // 2) * 2 + x % 2) * 4 + y


def step_pairs(step):
    dx, dy, dz = step
    return [
        (chip_index(x, y, z), chip_index((x + dx) % 4, (y + dy) % 4, (z + dz) % 8))
        for x in range(4)
        for y in range(4)
        for z in range(8)
    ]


def slot_towards(step):
    x = lax.axis_index("xl") + 4 + step[0]
    y = lax.axis_index("yl") + 4 + step[1]
    z = lax.axis_index("zl") + 4 + step[2]
    return lax.rem(x, 2) * 4 + lax.rem(z, 2) * 2 + lax.rem(y, 2)


def pack_kernel(steps, rows, at_ref, mask_ref, in_ref, grad_ref, *rest):
    out_refs, sem = rest[:-1], rest[-1]
    copies = []
    layers = []
    for k, out_ref in enumerate(out_refs):
        layer = at_ref[slot_towards(steps[k])]
        layers.append(layer)
        copies.append(
            pltpu.make_async_copy(in_ref.at[layer], out_ref.at[pl.ds(0, rows)], sem.at[k, 0])
        )
        copies.append(
            pltpu.make_async_copy(grad_ref.at[layer], out_ref.at[pl.ds(rows, rows)], sem.at[k, 1])
        )
    for copy in copies:
        copy.start()
    for layer, out_ref in zip(layers, out_refs):
        line = mask_ref[pl.ds(layer, 1), :].astype(jnp.float32)
        spare = jnp.zeros((MASK_ROWS, out_ref.shape[1] - rows), jnp.float32)
        wide = jnp.concatenate([jnp.broadcast_to(line, (MASK_ROWS, rows)), spare], axis=1)
        out_ref[2 * rows :, :] = wide.astype(jnp.bfloat16)
    for copy in copies:
        copy.wait()


def pack(steps, edge_in, edge_grad, row_mask, layer_at):
    _, rows, width = edge_in.shape
    piece = jax.ShapeDtypeStruct((2 * rows + MASK_ROWS, width), jnp.bfloat16)
    far = pl.BlockSpec(memory_space=pl.ANY)
    inside = pl.BlockSpec(memory_space=pltpu.VMEM)
    return pl.pallas_call(
        lambda *refs: pack_kernel(steps, rows, *refs),
        name="pack",
        compiler_params=pltpu.CompilerParams(vmem_limit_bytes=60 << 20),
        out_shape=(piece,) * len(steps),
        in_specs=[pl.BlockSpec(memory_space=pltpu.SMEM), inside, far, far],
        out_specs=(inside,) * len(steps),
        scratch_shapes=[pltpu.SemaphoreType.DMA((len(steps), 2))],
    )(layer_at, row_mask, edge_in, edge_grad)


def half_tiles(count):
    upper = upper_tiles(count)
    half = count // 2
    return [
        [("in", i, j) for i, j in upper]
        + [("grad", i, j) for i in range(half) for j in range(count)],
        [("out", i, j) for i, j in upper]
        + [("grad", i, j) for i in range(half, count) for j in range(count)],
    ]


def half_lines(width):
    return len(half_tiles(width // TILE)[0]) * TILE


def gram_kernel(pieces, rows, finish, refs):
    held_refs, refs = refs[:pieces], refs[pieces:]
    in_all, grad_all, mask_all, in_turned, grad_turned, sem = refs[-6:]
    width = in_all.shape[1]
    half = width // 2
    copies = []
    for k, held in enumerate(held_refs):
        at = pl.ds(k * rows, rows)
        copies.append(
            (
                pltpu.make_async_copy(held.at[pl.ds(0, rows)], in_all.at[at], sem.at[k, 0]),
                pltpu.make_async_copy(held.at[pl.ds(rows, rows)], grad_all.at[at], sem.at[k, 1]),
                pltpu.make_async_copy(
                    held.at[pl.ds(2 * rows, MASK_ROWS)], mask_all.at[k], sem.at[k, 2]
                ),
            )
        )
    for group in copies:
        for copy in group:
            copy.start()
    for k, group in enumerate(copies):
        for copy in group:
            copy.wait()
        at = slice(k * rows, (k + 1) * rows)
        in_turned[:, at] = in_all[at, :].T
        grad_turned[:, at] = grad_all[at, :].T
    weights = jnp.concatenate([mask_all[k, :1, :rows] for k in range(pieces)], axis=1)

    def dot(a, b):
        return jnp.dot(a, b, preferred_element_type=jnp.float32)

    finish(
        refs[:-6],
        2,
        ((slice(0, width), slice(0, width), dot(in_turned[...], grad_all[...])),),
    )
    for n, turned, plain in ((0, in_turned, in_all), (1, grad_turned, grad_all)):
        kept = turned[...] * weights
        upper, lower = slice(0, half), slice(half, width)
        finish(
            refs[:-6],
            n,
            (
                (upper, slice(0, width), dot(kept[:half], plain[...])),
                (lower, lower, dot(kept[half:], plain[:, half:])),
            ),
        )


def gram_scratch(pieces, rows, width):
    depth = pieces * rows
    return [
        pltpu.VMEM((depth, width), jnp.bfloat16),
        pltpu.VMEM((depth, width), jnp.bfloat16),
        pltpu.VMEM((pieces, MASK_ROWS, width), jnp.bfloat16),
        pltpu.VMEM((width, depth), jnp.bfloat16),
        pltpu.VMEM((width, depth), jnp.bfloat16),
        pltpu.SemaphoreType.DMA((pieces, 3)),
    ]


def gram_some(held, rows, *before):
    width = held[0].shape[1]
    anywhere = pl.BlockSpec(memory_space=pl.ANY)
    inside = pl.BlockSpec(memory_space=pltpu.VMEM)

    def kernel(*refs):
        sums, refs = refs[: len(before)], refs[len(before) :]

        def keep(outs, n, blocks):
            for at, to, value in blocks:
                for ref in sums:
                    value = value + ref[n, at, to]
                outs[0][n, at, to] = value

        gram_kernel(len(held), rows, keep, refs)

    return pl.pallas_call(
        kernel,
        name="gram_some",
        compiler_params=pltpu.CompilerParams(vmem_limit_bytes=28 << 20),
        out_shape=jax.ShapeDtypeStruct((3, width, width), jnp.float32),
        in_specs=[inside] * len(before) + [anywhere] * len(held),
        out_specs=inside,
        scratch_shapes=gram_scratch(len(held), rows, width),
    )(*before, *held)


def gram_last(sums, held, rows, rows_all):
    width = held[0].shape[1]
    lines = half_lines(width)
    halves = half_tiles(width // TILE)
    scales = (1.0 / rows_all, 1.0 / rows_all, 1.0 / math.sqrt(rows_all))
    kinds = ("in", "out", "grad")
    inside = pl.BlockSpec(memory_space=pltpu.VMEM)
    anywhere = pl.BlockSpec(memory_space=pl.ANY)

    def kernel(*refs):
        pieces = len(held)
        sums_ref = refs[0]

        def write(outs, n, blocks):
            mine_ref, theirs_ref, whole_ref = outs
            for at, to, value in blocks:
                whole_ref[n, at, to] = sums_ref[n, at, to] + value
            for core in range(2):

                @pl.when(lax.axis_index("core") == core)
                def _(core=core):
                    for ref, tiles in ((mine_ref, halves[core]), (theirs_ref, halves[1 - core])):
                        for spot, (kind, i, j) in enumerate(tiles):
                            if kind == kinds[n]:
                                across = slice(j * TILE, (j + 1) * TILE)
                                tile = whole_ref[n, i * TILE : (i + 1) * TILE, across] * scales[n]
                                ref[spot * TILE : (spot + 1) * TILE, :] = tile.astype(ref.dtype)

        gram_kernel(pieces, rows, write, refs[1:])

    return pl.pallas_call(
        kernel,
        name="gram_last",
        compiler_params=pltpu.CompilerParams(vmem_limit_bytes=28 << 20),
        out_shape=(
            jax.ShapeDtypeStruct((lines, TILE), jnp.float32),
            jax.ShapeDtypeStruct((lines, TILE), jnp.bfloat16),
        ),
        in_specs=[inside] + [anywhere] * len(held),
        out_specs=(inside, inside),
        scratch_shapes=[pltpu.VMEM((3, width, width), jnp.float32)]
        + gram_scratch(len(held), rows, width),
    )(sums, *held)


def pair_kernel(mine_ref, other_ref, *out_refs):
    here = lax.axis_index("xh") * 2 + lax.axis_index("yh")
    lines = out_refs[0].shape[0]
    for k, ref in enumerate(out_refs):
        at = pl.ds(pl.multiple_of((here ^ k) * lines, lines), lines)
        ref[...] = (mine_ref[at, :] + other_ref[at, :].astype(jnp.float32)).astype(ref.dtype)


def pair_sum(mine, other):
    inside = pl.BlockSpec(memory_space=pltpu.VMEM)
    shape = (mine.shape[0] // 4, TILE)
    return pl.pallas_call(
        pair_kernel,
        name="pair",
        compiler_params=pltpu.CompilerParams(vmem_limit_bytes=8 << 20),
        out_shape=[jax.ShapeDtypeStruct(shape, jnp.float32)]
        + [jax.ShapeDtypeStruct(shape, jnp.bfloat16)] * 3,
        in_specs=[inside, inside],
        out_specs=[inside] * 4,
    )(mine, other)


def quarter_kernel(own_ref, *refs):
    whole = own_ref[...]
    for ref in refs[:-1]:
        whole += ref[...].astype(jnp.float32)
    refs[-1][...] = whole.astype(jnp.bfloat16)


def quarter_sum(own, others):
    inside = pl.BlockSpec(memory_space=pltpu.VMEM)
    return pl.pallas_call(
        quarter_kernel,
        name="quarter",
        compiler_params=pltpu.CompilerParams(vmem_limit_bytes=8 << 20),
        out_shape=jax.ShapeDtypeStruct(own.shape, jnp.bfloat16),
        in_specs=[inside] * (1 + len(others)),
        out_specs=inside,
    )(own, *others)


def total_kernel(arrived_ref, out_ref):
    count = arrived_ref.shape[0]
    for slot in range(2):
        whole = arrived_ref[slot].astype(jnp.float32)
        for k in range(slot + 2, count, 2):
            whole += arrived_ref[k].astype(jnp.float32)
        low = whole.astype(jnp.bfloat16)
        for k in range(out_ref.shape[0]):
            if k // count % 2 == slot:
                out_ref[k] = low


def total(arrived):
    count, lines, _ = arrived.shape
    return pl.pallas_call(
        total_kernel,
        name="total",
        compiler_params=pltpu.CompilerParams(vmem_limit_bytes=8 << 20),
        out_shape=jax.ShapeDtypeStruct((4 * count, lines, TILE), arrived.dtype),
        in_specs=[pl.BlockSpec(memory_space=pltpu.VMEM)],
        out_specs=pl.BlockSpec(memory_space=pltpu.VMEM),
    )(arrived)


def diagonal_of_tile():
    rows = lax.broadcasted_iota(jnp.int32, (TILE, TILE), 0)
    return rows == lax.broadcasted_iota(jnp.int32, (TILE, TILE), 1)


def low_dot(a, b):
    return jnp.dot(a, b, preferred_element_type=jnp.float32)


def powers(tiles_ref, whole_ref, put):
    width = whole_ref.shape[0]
    count = width // TILE
    diagonal = diagonal_of_tile()
    trace = jnp.zeros((TILE, TILE), jnp.float32)
    for spot, (i, j) in enumerate(upper_tiles(count)):
        tile = tiles_ref[spot * TILE : (spot + 1) * TILE, :].astype(jnp.float32)
        whole_ref[i * TILE : (i + 1) * TILE, j * TILE : (j + 1) * TILE] = tile
        if i == j:
            trace += jnp.where(diagonal, tile, 0.0)
        else:
            whole_ref[j * TILE : (j + 1) * TILE, i * TILE : (i + 1) * TILE] = tile.T
    shift = jnp.where(diagonal, jnp.sum(trace) * (0.05 / width), 0.0)
    for i in range(count):
        at = slice(i * TILE, (i + 1) * TILE)
        whole_ref[at, at] += shift
    whole = whole_ref[...]
    scale = lax.rsqrt(jnp.sum(whole * whole) + 1e-06)
    whole = whole * scale
    for step in range(ITERS):
        low = whole.astype(jnp.bfloat16)
        put(step, low)
        if step < ITERS - 1:
            whole = 2.0 * whole - low_dot(low, low)
    return scale


def own_powers_kernel(own_ref, out_ref, scale_ref, whole_ref):
    def put(step, low):
        out_ref[step] = low

    scale_ref[...] = jnp.full(scale_ref.shape, powers(own_ref, whole_ref, put))


def own_powers(own, width):
    inside = pl.BlockSpec(memory_space=pltpu.VMEM)
    return pl.pallas_call(
        own_powers_kernel,
        name="own_powers",
        compiler_params=pltpu.CompilerParams(vmem_limit_bytes=12 << 20),
        out_shape=(
            jax.ShapeDtypeStruct((ITERS, width, width), jnp.bfloat16),
            jax.ShapeDtypeStruct((8, TILE), jnp.float32),
        ),
        in_specs=[inside],
        out_specs=(inside, inside),
        scratch_shapes=[pltpu.VMEM((width, width), jnp.float32)],
    )(own)


def newton_kernel(
    scale_ref, mine_ref, own_ref, other_ref, out_ref, all_ref, whole_ref, mid_ref, sem
):
    width = whole_ref.shape[0]
    count = width // TILE
    core = lax.axis_index("core")
    bring = pltpu.make_async_copy(mine_ref, all_ref.at[0], sem)
    bring.start()

    def put(step, low):
        all_ref[1, step] = low

    scale = powers(other_ref, whole_ref, put) * scale_ref[:1, :1]
    base = len(upper_tiles(count)) * TILE
    half = count // 2
    for part, ref in enumerate((own_ref, other_ref)):
        first = jnp.where(core == part, 0, half * TILE)
        for i in range(half):
            for j in range(count):
                spot = base + (i * count + j) * TILE
                at = pl.ds(pl.multiple_of(first + i * TILE, TILE), TILE)
                mid_ref[at, j * TILE : (j + 1) * TILE] = ref[spot : spot + TILE, :].astype(
                    jnp.float32
                )
    bring.wait()
    cut = width // 2
    parts = [mid_ref[:, :cut], mid_ref[:, cut:]]
    for step in range(ITERS):
        left = all_ref[core, step]
        parts = [2.0 * part - low_dot(left, part.astype(jnp.bfloat16)) for part in parts]
    whole = jnp.concatenate(parts, axis=1)
    parts = [whole[:cut], whole[cut:]]
    for step in range(ITERS):
        right = all_ref[1 - core, step]
        parts = [2.0 * part - low_dot(part.astype(jnp.bfloat16), right) for part in parts]
    out_ref[:cut, :] = (parts[0] * scale).astype(jnp.bfloat16)
    out_ref[cut:, :] = (parts[1] * scale).astype(jnp.bfloat16)


def newton(scale, mine, own, other, width):
    inside = pl.BlockSpec(memory_space=pltpu.VMEM)
    return pl.pallas_call(
        newton_kernel,
        name="newton",
        compiler_params=pltpu.CompilerParams(vmem_limit_bytes=20 << 20),
        out_shape=jax.ShapeDtypeStruct((width, width), jnp.bfloat16),
        in_specs=[inside, pl.BlockSpec(memory_space=pl.ANY), inside, inside],
        out_specs=inside,
        scratch_shapes=[
            pltpu.VMEM((2, ITERS, width, width), jnp.bfloat16),
            pltpu.VMEM((width, width), jnp.float32),
            pltpu.VMEM((width, width), jnp.float32),
            pltpu.SemaphoreType.DMA,
        ],
    )(scale, mine, own, other)


def local(edge_in, edge_grad, row_mask, layer_at):
    rows = edge_in.shape[1]
    width = edge_in.shape[2]
    rows_all = rows * lax.axis_size(AXES)
    swap = [(0, 1), (1, 0)]
    args = (edge_in, edge_grad, row_mask, layer_at)

    def exchanged(sent, steps):
        return [lax.ppermute(p, CHIPS, step_pairs(step)) for p, step in zip(sent, steps)]

    early = exchanged(pack(FIRST, *args), FIRST)
    *sent, kept = pack(SECOND + (HERE,), *args)
    late = exchanged(sent, SECOND)
    sums = gram_some([kept] + early, rows)
    sums = gram_some(late[:-1], rows, sums)
    mine, theirs = gram_last(sums, late[-1:], rows, rows_all)
    here, *away = pair_sum(mine, lax.ppermute(theirs, "core", swap))
    came = [
        lax.ppermute(part, ("xh", "yh"), [(i, i ^ (k + 1)) for i in range(4)])
        for k, part in reversed(list(enumerate(away)))
    ]
    blocks = quarter_sum(here, came).reshape(lax.axis_size(("zh", "zl")), -1, TILE)
    arrived = lax.all_to_all(blocks, ("zh", "zl"), 0, 0, tiled=True)
    around = ("xh", "yh", "zh", "zl")
    own = lax.all_to_all(total(arrived), around, 0, 0, tiled=True).reshape(-1, TILE)
    other = lax.ppermute(own, "core", swap)
    low, scale = own_powers(own, width)
    update = newton(scale, low, own, other, width)
    return update[None]


def solution(mesh):
    split = Mesh(mesh.devices.reshape(tuple(SIZES[a] for a in AXES)), AXES)
    placed = (P(None, AXES, None), P(None, AXES, None), P(None, AXES), P())
    return jax.shard_map(
        local, mesh=split, in_specs=placed, out_specs=P(OWNER, None, None), check_vma=False
    )
```

```python
import math

import jax
import jax.numpy as jnp
from jax import lax
from jax.experimental import pallas as pl
from jax.experimental.pallas import tpu as pltpu
from jax.sharding import Mesh
from jax.sharding import PartitionSpec as P

ITERS = 4
AXES = ("zh", "zl", "xh", "core", "xl", "yh", "yl")
CHIPS = ("zh", "zl", "xh", "xl", "yh", "yl")
OWNER = ("xl", "yh", "yl")
SIZES = {"zh": 4, "zl": 2, "xh": 2, "core": 2, "xl": 2, "yh": 2, "yl": 2}
FIRST = ((1, 0, 0), (0, 0, 1), (0, 1, 0), (-1, -1, -1))
SECOND = ((1, -1, 0), (-1, 0, 1), (0, 1, -1))
HERE = (0, 0, 0)
MASK_ROWS = 8
TILE = 128


def upper_tiles(count):
    return [(i, j) for i in range(count) for j in range(i, count)]


def chip_index(x, y, z):
    return ((z * 2 + x // 2) * 2 + x % 2) * 4 + y


def step_pairs(step):
    dx, dy, dz = step
    return [
        (chip_index(x, y, z), chip_index((x + dx) % 4, (y + dy) % 4, (z + dz) % 8))
        for x in range(4)
        for y in range(4)
        for z in range(8)
    ]


def slot_towards(step):
    x = lax.axis_index("xl") + 4 + step[0]
    y = lax.axis_index("yl") + 4 + step[1]
    z = lax.axis_index("zl") + 4 + step[2]
    return lax.rem(x, 2) * 4 + lax.rem(z, 2) * 2 + lax.rem(y, 2)


def pack_kernel(steps, rows, at_ref, mask_ref, in_ref, grad_ref, *rest):
    out_refs, sem = rest[:-1], rest[-1]
    copies = []
    layers = []
    for k, out_ref in enumerate(out_refs):
        layer = at_ref[slot_towards(steps[k])]
        layers.append(layer)
        copies.append(
            pltpu.make_async_copy(in_ref.at[layer], out_ref.at[pl.ds(0, rows)], sem.at[k, 0])
        )
        copies.append(
            pltpu.make_async_copy(grad_ref.at[layer], out_ref.at[pl.ds(rows, rows)], sem.at[k, 1])
        )
    for copy in copies:
        copy.start()
    for layer, out_ref in zip(layers, out_refs):
        line = mask_ref[pl.ds(layer, 1), :].astype(jnp.float32)
        spare = jnp.zeros((MASK_ROWS, out_ref.shape[1] - rows), jnp.float32)
        wide = jnp.concatenate([jnp.broadcast_to(line, (MASK_ROWS, rows)), spare], axis=1)
        out_ref[2 * rows :, :] = wide.astype(jnp.bfloat16)
    for copy in copies:
        copy.wait()


def pack(steps, edge_in, edge_grad, row_mask, layer_at):
    _, rows, width = edge_in.shape
    piece = jax.ShapeDtypeStruct((2 * rows + MASK_ROWS, width), jnp.bfloat16)
    far = pl.BlockSpec(memory_space=pl.ANY)
    inside = pl.BlockSpec(memory_space=pltpu.VMEM)
    return pl.pallas_call(
        lambda *refs: pack_kernel(steps, rows, *refs),
        name="pack",
        compiler_params=pltpu.CompilerParams(vmem_limit_bytes=60 << 20),
        out_shape=(piece,) * len(steps),
        in_specs=[pl.BlockSpec(memory_space=pltpu.SMEM), inside, far, far],
        out_specs=(inside,) * len(steps),
        scratch_shapes=[pltpu.SemaphoreType.DMA((len(steps), 2))],
    )(layer_at, row_mask, edge_in, edge_grad)


def half_tiles(count):
    upper = upper_tiles(count)
    half = count // 2
    return [
        [("in", i, j) for i, j in upper]
        + [("grad", i, j) for i in range(half) for j in range(count)],
        [("out", i, j) for i, j in upper]
        + [("grad", i, j) for i in range(half, count) for j in range(count)],
    ]


def half_lines(width):
    return len(half_tiles(width // TILE)[0]) * TILE


def gram_kernel(pieces, rows, finish, refs):
    held_refs, refs = refs[:pieces], refs[pieces:]
    in_all, grad_all, mask_all, in_turned, grad_turned, sem = refs[-6:]
    width = in_all.shape[1]
    half = width // 2
    copies = []
    for k, held in enumerate(held_refs):
        at = pl.ds(k * rows, rows)
        copies.append(
            (
                pltpu.make_async_copy(held.at[pl.ds(0, rows)], in_all.at[at], sem.at[k, 0]),
                pltpu.make_async_copy(held.at[pl.ds(rows, rows)], grad_all.at[at], sem.at[k, 1]),
                pltpu.make_async_copy(
                    held.at[pl.ds(2 * rows, MASK_ROWS)], mask_all.at[k], sem.at[k, 2]
                ),
            )
        )
    for group in copies:
        for copy in group:
            copy.start()
    for k, group in enumerate(copies):
        for copy in group:
            copy.wait()
        at = slice(k * rows, (k + 1) * rows)
        in_turned[:, at] = in_all[at, :].T
        grad_turned[:, at] = grad_all[at, :].T
    weights = jnp.concatenate([mask_all[k, :1, :rows] for k in range(pieces)], axis=1)

    def dot(a, b):
        return jnp.dot(a, b, preferred_element_type=jnp.float32)

    finish(
        refs[:-6],
        2,
        ((slice(0, width), slice(0, width), dot(in_turned[...], grad_all[...])),),
    )
    for n, turned, plain in ((0, in_turned, in_all), (1, grad_turned, grad_all)):
        kept = turned[...] * weights
        upper, lower = slice(0, half), slice(half, width)
        finish(
            refs[:-6],
            n,
            (
                (upper, slice(0, width), dot(kept[:half], plain[...])),
                (lower, lower, dot(kept[half:], plain[:, half:])),
            ),
        )


def gram_scratch(pieces, rows, width):
    depth = pieces * rows
    return [
        pltpu.VMEM((depth, width), jnp.bfloat16),
        pltpu.VMEM((depth, width), jnp.bfloat16),
        pltpu.VMEM((pieces, MASK_ROWS, width), jnp.bfloat16),
        pltpu.VMEM((width, depth), jnp.bfloat16),
        pltpu.VMEM((width, depth), jnp.bfloat16),
        pltpu.SemaphoreType.DMA((pieces, 3)),
    ]


def gram_some(held, rows, *before):
    width = held[0].shape[1]
    anywhere = pl.BlockSpec(memory_space=pl.ANY)
    inside = pl.BlockSpec(memory_space=pltpu.VMEM)

    def kernel(*refs):
        sums, refs = refs[: len(before)], refs[len(before) :]

        def keep(outs, n, blocks):
            for at, to, value in blocks:
                for ref in sums:
                    value = value + ref[n, at, to]
                outs[0][n, at, to] = value

        gram_kernel(len(held), rows, keep, refs)

    return pl.pallas_call(
        kernel,
        name="gram_some",
        compiler_params=pltpu.CompilerParams(vmem_limit_bytes=28 << 20),
        out_shape=jax.ShapeDtypeStruct((3, width, width), jnp.float32),
        in_specs=[inside] * len(before) + [anywhere] * len(held),
        out_specs=inside,
        scratch_shapes=gram_scratch(len(held), rows, width),
    )(*before, *held)


def gram_last(sums, held, rows, rows_all):
    width = held[0].shape[1]
    lines = half_lines(width)
    halves = half_tiles(width // TILE)
    scales = (1.0 / rows_all, 1.0 / rows_all, 1.0 / math.sqrt(rows_all))
    kinds = ("in", "out", "grad")
    inside = pl.BlockSpec(memory_space=pltpu.VMEM)
    anywhere = pl.BlockSpec(memory_space=pl.ANY)

    def kernel(*refs):
        pieces = len(held)
        sums_ref = refs[0]

        def write(outs, n, blocks):
            mine_ref, theirs_ref, whole_ref = outs
            for at, to, value in blocks:
                whole_ref[n, at, to] = sums_ref[n, at, to] + value
            for core in range(2):

                @pl.when(lax.axis_index("core") == core)
                def _(core=core):
                    for ref, tiles in ((mine_ref, halves[core]), (theirs_ref, halves[1 - core])):
                        for spot, (kind, i, j) in enumerate(tiles):
                            if kind == kinds[n]:
                                across = slice(j * TILE, (j + 1) * TILE)
                                tile = whole_ref[n, i * TILE : (i + 1) * TILE, across] * scales[n]
                                ref[spot * TILE : (spot + 1) * TILE, :] = tile.astype(ref.dtype)

        gram_kernel(pieces, rows, write, refs[1:])

    return pl.pallas_call(
        kernel,
        name="gram_last",
        compiler_params=pltpu.CompilerParams(vmem_limit_bytes=28 << 20),
        out_shape=(
            jax.ShapeDtypeStruct((lines, TILE), jnp.float32),
            jax.ShapeDtypeStruct((lines, TILE), jnp.bfloat16),
        ),
        in_specs=[inside] + [anywhere] * len(held),
        out_specs=(inside, inside),
        scratch_shapes=[pltpu.VMEM((3, width, width), jnp.float32)]
        + gram_scratch(len(held), rows, width),
    )(sums, *held)


def pair_kernel(mine_ref, other_ref, *out_refs):
    here = lax.axis_index("xh") * 2 + lax.axis_index("yh")
    lines = out_refs[0].shape[0]
    for k, ref in enumerate(out_refs):
        at = pl.ds(pl.multiple_of((here ^ k) * lines, lines), lines)
        ref[...] = (mine_ref[at, :] + other_ref[at, :].astype(jnp.float32)).astype(ref.dtype)


def pair_sum(mine, other):
    inside = pl.BlockSpec(memory_space=pltpu.VMEM)
    shape = (mine.shape[0] // 4, TILE)
    return pl.pallas_call(
        pair_kernel,
        name="pair",
        compiler_params=pltpu.CompilerParams(vmem_limit_bytes=8 << 20),
        out_shape=[jax.ShapeDtypeStruct(shape, jnp.float32)]
        + [jax.ShapeDtypeStruct(shape, jnp.bfloat16)] * 3,
        in_specs=[inside, inside],
        out_specs=[inside] * 4,
    )(mine, other)


def quarter_kernel(own_ref, *refs):
    whole = own_ref[...]
    for ref in refs[:-1]:
        whole += ref[...].astype(jnp.float32)
    refs[-1][...] = whole.astype(jnp.bfloat16)


def quarter_sum(own, others):
    inside = pl.BlockSpec(memory_space=pltpu.VMEM)
    return pl.pallas_call(
        quarter_kernel,
        name="quarter",
        compiler_params=pltpu.CompilerParams(vmem_limit_bytes=8 << 20),
        out_shape=jax.ShapeDtypeStruct(own.shape, jnp.bfloat16),
        in_specs=[inside] * (1 + len(others)),
        out_specs=inside,
    )(own, *others)


def total_kernel(arrived_ref, out_ref):
    count = arrived_ref.shape[0]
    for slot in range(2):
        whole = arrived_ref[slot].astype(jnp.float32)
        for k in range(slot + 2, count, 2):
            whole += arrived_ref[k].astype(jnp.float32)
        low = whole.astype(jnp.bfloat16)
        for k in range(out_ref.shape[0]):
            if k // count % 2 == slot:
                out_ref[k] = low


def total(arrived):
    count, lines, _ = arrived.shape
    return pl.pallas_call(
        total_kernel,
        name="total",
        compiler_params=pltpu.CompilerParams(vmem_limit_bytes=8 << 20),
        out_shape=jax.ShapeDtypeStruct((4 * count, lines, TILE), arrived.dtype),
        in_specs=[pl.BlockSpec(memory_space=pltpu.VMEM)],
        out_specs=pl.BlockSpec(memory_space=pltpu.VMEM),
    )(arrived)


def diagonal_of_tile():
    rows = lax.broadcasted_iota(jnp.int32, (TILE, TILE), 0)
    return rows == lax.broadcasted_iota(jnp.int32, (TILE, TILE), 1)


def low_dot(a, b):
    return jnp.dot(a, b, preferred_element_type=jnp.float32)


def powers(tiles_ref, whole_ref, put):
    width = whole_ref.shape[0]
    count = width // TILE
    diagonal = diagonal_of_tile()
    trace = jnp.zeros((TILE, TILE), jnp.float32)
    for spot, (i, j) in enumerate(upper_tiles(count)):
        tile = tiles_ref[spot * TILE : (spot + 1) * TILE, :].astype(jnp.float32)
        whole_ref[i * TILE : (i + 1) * TILE, j * TILE : (j + 1) * TILE] = tile
        if i == j:
            trace += jnp.where(diagonal, tile, 0.0)
        else:
            whole_ref[j * TILE : (j + 1) * TILE, i * TILE : (i + 1) * TILE] = tile.T
    shift = jnp.where(diagonal, jnp.sum(trace) * (0.05 / width), 0.0)
    for i in range(count):
        at = slice(i * TILE, (i + 1) * TILE)
        whole_ref[at, at] += shift
    whole = whole_ref[...]
    scale = lax.rsqrt(jnp.sum(whole * whole) + 1e-06)
    whole = whole * scale
    for step in range(ITERS):
        low = whole.astype(jnp.bfloat16)
        put(step, low)
        if step < ITERS - 1:
            whole = 2.0 * whole - low_dot(low, low)
    return scale


def own_powers_kernel(own_ref, out_ref, scale_ref, whole_ref):
    def put(step, low):
        out_ref[step] = low

    scale_ref[...] = jnp.full(scale_ref.shape, powers(own_ref, whole_ref, put))


def own_powers(own, width):
    inside = pl.BlockSpec(memory_space=pltpu.VMEM)
    return pl.pallas_call(
        own_powers_kernel,
        name="own_powers",
        compiler_params=pltpu.CompilerParams(vmem_limit_bytes=12 << 20),
        out_shape=(
            jax.ShapeDtypeStruct((ITERS, width, width), jnp.bfloat16),
            jax.ShapeDtypeStruct((8, TILE), jnp.float32),
        ),
        in_specs=[inside],
        out_specs=(inside, inside),
        scratch_shapes=[pltpu.VMEM((width, width), jnp.float32)],
    )(own)


def newton_kernel(
    scale_ref, mine_ref, own_ref, other_ref, out_ref, all_ref, whole_ref, mid_ref, sem
):
    width = whole_ref.shape[0]
    count = width // TILE
    core = lax.axis_index("core")
    bring = pltpu.make_async_copy(mine_ref, all_ref.at[0], sem)
    bring.start()

    def put(step, low):
        all_ref[1, step] = low

    scale = powers(other_ref, whole_ref, put) * scale_ref[:1, :1]
    base = len(upper_tiles(count)) * TILE
    half = count // 2
    for part, ref in enumerate((own_ref, other_ref)):
        first = jnp.where(core == part, 0, half * TILE)
        for i in range(half):
            for j in range(count):
                spot = base + (i * count + j) * TILE
                at = pl.ds(pl.multiple_of(first + i * TILE, TILE), TILE)
                mid_ref[at, j * TILE : (j + 1) * TILE] = ref[spot : spot + TILE, :].astype(
                    jnp.float32
                )
    bring.wait()
    cut = width // 2
    parts = [mid_ref[:, :cut], mid_ref[:, cut:]]
    for step in range(ITERS):
        left = all_ref[core, step]
        parts = [2.0 * part - low_dot(left, part.astype(jnp.bfloat16)) for part in parts]
    whole = jnp.concatenate(parts, axis=1)
    parts = [whole[:cut], whole[cut:]]
    for step in range(ITERS):
        right = all_ref[1 - core, step]
        parts = [2.0 * part - low_dot(part.astype(jnp.bfloat16), right) for part in parts]
    out_ref[:cut, :] = (parts[0] * scale).astype(jnp.bfloat16)
    out_ref[cut:, :] = (parts[1] * scale).astype(jnp.bfloat16)


def newton(scale, mine, own, other, width):
    inside = pl.BlockSpec(memory_space=pltpu.VMEM)
    return pl.pallas_call(
        newton_kernel,
        name="newton",
        compiler_params=pltpu.CompilerParams(vmem_limit_bytes=20 << 20),
        out_shape=jax.ShapeDtypeStruct((width, width), jnp.bfloat16),
        in_specs=[inside, pl.BlockSpec(memory_space=pl.ANY), inside, inside],
        out_specs=inside,
        scratch_shapes=[
            pltpu.VMEM((2, ITERS, width, width), jnp.bfloat16),
            pltpu.VMEM((width, width), jnp.float32),
            pltpu.VMEM((width, width), jnp.float32),
            pltpu.SemaphoreType.DMA,
        ],
    )(scale, mine, own, other)


def local(edge_in, edge_grad, row_mask, layer_at):
    rows = edge_in.shape[1]
    width = edge_in.shape[2]
    rows_all = rows * lax.axis_size(AXES)
    swap = [(0, 1), (1, 0)]
    args = (edge_in, edge_grad, row_mask, layer_at)

    def exchanged(sent, steps):
        return [lax.ppermute(p, CHIPS, step_pairs(step)) for p, step in zip(sent, steps)]

    early = exchanged(pack(FIRST, *args), FIRST)
    *sent, kept = pack(SECOND + (HERE,), *args)
    late = exchanged(sent, SECOND)
    sums = gram_some([kept] + early, rows)
    sums = gram_some(late[:-1], rows, sums)
    mine, theirs = gram_last(sums, late[-1:], rows, rows_all)
    here, *away = pair_sum(mine, lax.ppermute(theirs, "core", swap))
    came = [
        lax.ppermute(part, ("xh", "yh"), [(i, i ^ (k + 1)) for i in range(4)])
        for k, part in enumerate(away)
    ]
    blocks = quarter_sum(here, came).reshape(lax.axis_size(("zh", "zl")), -1, TILE)
    arrived = lax.all_to_all(blocks, ("zh", "zl"), 0, 0, tiled=True)
    around = ("xh", "yh", "zh", "zl")
    own = lax.all_to_all(total(arrived), around, 0, 0, tiled=True).reshape(-1, TILE)
    other = lax.ppermute(own, "core", swap)
    low, scale = own_powers(own, width)
    update = newton(scale, low, own, other, width)
    return update[None]


def solution(mesh):
    split = Mesh(mesh.devices.reshape(tuple(SIZES[a] for a in AXES)), AXES)
    placed = (P(None, AXES, None), P(None, AXES, None), P(None, AXES), P())
    return jax.shard_map(
        local, mesh=split, in_specs=placed, out_specs=P(OWNER, None, None), check_vma=False
    )
```
